256 devices in a mesh: samples: 4 (over x), features: 32 (over z, y), rhs: 2 (over core).
Axes of the slice: x: 4, y: 4, z: 8, core: 2. Of those that a mesh axis runs over, the one named last changes fastest.
Arguments:
- design: bfloat16 [32768, 32768], P(('samples', 'rhs'), 'features'), may hold values from -0.03125 to 0.03125
- right_side: float32 [32768, 64], P('features', 'rhs'), may hold values from -6 to 6
- factor: bfloat16 [32768, 768], P('features', 'rhs'), may hold values from -0.03125 to 0.03125
- nystrom_values: float32 [768], replicated, may hold values from 0.5 to 3
Outputs:
- solution: float32 [32768, 64], P('features', 'rhs')
- residual: float32 [32768, 64], P('features', 'rhs')
The draws below stay inside these ranges and needn't reach their ends.
All inputs are finite; a program needn't handle non-finite values.
Results may differ from the reference program's by a relative error of at most 0.0181.
Values may be sent and summed in bfloat16 or wider, within the bound.
A program may use at most 64 MiB of HBM per device.

```python
import math
import jax
import jax.numpy as jnp
from jax import lax

F = 32768
K = 64
R = 768
ITERS = 3
NS = 32768


def block_levels(key, shape, cuts, low, top_value):
    level, own = 1.0, jax.random.fold_in(key, 6)
    for dim, shards_of in cuts:
        steps = jnp.exp(jax.random.uniform(jax.random.fold_in(own, dim), (shards_of,), jnp.float32, low / len(cuts), top_value / len(cuts)))
        level = level * jnp.repeat(steps, shape[dim] // shards_of).reshape([-1 if axis == dim else 1 for axis in range(len(shape))])
    return level


def scatter_about(rng, extent, deviation, most, pieces=(), held_as=jnp.bfloat16):
    factor_of = block_levels(rng, extent, pieces, -0.22, 0.18) if pieces else 1.0
    array = jax.random.normal(rng, extent, jnp.float32) * deviation * factor_of
    return jnp.minimum(jnp.maximum(array, -most), most).astype(held_as)


def setup_inputs(seed: int = 0) -> dict:
    splits = jax.random.split(jax.random.key(seed), 5)
    design = scatter_about(splits[0], (NS, F), NS ** -0.5, 0.03125, ((0, 8), (1, 32)))
    right_side = scatter_about(splits[1], (F, K), 1.0, 6.0, ((0, 32), (1, 2)), jnp.float32)
    factor = scatter_about(splits[2], (F, R), F ** -0.5, 0.03125, ((0, 32), (1, 2)))
    nystrom_values = jnp.clip(jnp.exp(jax.random.uniform(splits[3], (R,), jnp.float32, math.log(0.5), math.log(3.0))), 0.5, 3.0)
    return {"design": design, "right_side": right_side, "factor": factor, "nystrom_values": nystrom_values}


ridge_weight = 1.0

def inner_prod(left, right):
    return lax.dot_general(left.astype(jnp.float32), right.astype(jnp.float32), (((0,), (0,)), ((), ())), precision=lax.Precision.HIGHEST, preferred_element_type=jnp.float32)

def apply_operator(design, direction):
    narrow = direction.astype(jnp.bfloat16)
    images = jnp.dot(design.astype(jnp.float32), narrow.astype(jnp.float32), preferred_element_type=jnp.float32).astype(jnp.bfloat16)
    summed = lax.dot_general(design.astype(jnp.float32), images.astype(jnp.float32), (((0,), (0,)), ((), ())), preferred_element_type=jnp.float32)
    return summed + ridge_weight * direction

def reference(design, right_side, factor, nystrom_values):
    shrink = (1.0 + jnp.min(nystrom_values)) / (1.0 + nystrom_values) - 1.0
    factor_wide = factor.astype(jnp.float32)

    def precondition(values):
        projected = inner_prod(factor_wide, values)
        return values + jnp.dot(factor_wide, shrink[:, None] * projected, precision=lax.Precision.HIGHEST)
    solution = jnp.zeros_like(right_side)
    residual = right_side
    direction = precondition(residual)
    for iteration in range(ITERS):
        applied = apply_operator(design, direction)
        gram_block = inner_prod(direction, applied)
        gram_block = 0.5 * (gram_block + gram_block.T)
        chol_lower = jnp.linalg.cholesky(gram_block)
        unit_dir = jax.scipy.linalg.solve_triangular(chol_lower, direction.T, lower=True).T
        unit_img = jax.scipy.linalg.solve_triangular(chol_lower, applied.T, lower=True).T
        step_coef = jax.scipy.linalg.solve_triangular(chol_lower, inner_prod(direction, residual), lower=True)
        solution = solution + jnp.dot(unit_dir, step_coef, precision=lax.Precision.HIGHEST)
        residual = residual - jnp.dot(unit_img, step_coef, precision=lax.Precision.HIGHEST)
        if iteration + 1 < ITERS:
            scaled = precondition(residual)
            next_coef = -inner_prod(unit_img, scaled)
            direction = scaled + jnp.dot(unit_dir, next_coef, precision=lax.Precision.HIGHEST)
    return (solution, residual)
```

```python
import functools

import jax
import jax.numpy as jnp
from jax import lax
from jax.experimental import pallas as pl
from jax.experimental.pallas import tpu as pltpu
from jax.sharding import PartitionSpec as P

ITERS = 3
LANES = 128
MESH = pl.DeviceIdType.MESH
F32 = jnp.float32
BF16 = jnp.bfloat16
WIRE = jnp.float32


def nt(a, b):
    return lax.dot_general(a, b, (((1,), (1,)), ((), ())), preferred_element_type=F32)


def nn(a, b):
    return lax.dot_general(a, b, (((1,), (0,)), ((), ())), preferred_element_type=F32)


def halves(v):
    upper = v.astype(BF16)
    lower = (v - upper.astype(F32)).astype(BF16)
    return upper, lower


def nn_fine(a, b):
    ah, al = halves(a)
    bh, bl = halves(b)
    return nn(jnp.concatenate([ah, ah, al, al], 1), jnp.concatenate([bh, bl, bh, bl], 0))


def nt_fine(a, b):
    m, n = a.shape[0], b.shape[0]
    t = nt(jnp.concatenate(halves(a), 0), jnp.concatenate(halves(b), 0))
    return t[:m, :n] + t[:m, n:] + t[m:, :n] + t[m:, n:]


def rows_fine(a, op, b):
    m = a.shape[0]
    t = op(jnp.concatenate(halves(a), 0), b)
    return t[:m] + t[m:]


def inverse(a):
    n = a.shape[0]
    lane = lax.broadcasted_iota(jnp.int32, (1, n), 1)
    sub = lax.broadcasted_iota(jnp.int32, (n, 1), 0)
    for i in range(n):
        pivot = 1.0 / a[i : i + 1, i : i + 1]
        row = jnp.where(lane == i, 1.0, a[i : i + 1, :]) * pivot
        col = a[:, i : i + 1]
        rest = jnp.where(lane == i, 0.0, a) - col * row
        a = jnp.where(sub == i, row, rest)
    return a


def kernel(
    dims,
    d_hbm, rt_in, f_in, shrink,
    x_out, r_out,
    dv, rfull, fall, pt, rt, xt, yt, ginv, qt,
    s1, r1, acc1, s2, r2, own2, img, qacc,
    gxs, gxr, gyr, gzr, gall,
    qds, qdr, qxr, qf,
    wyr, wzr, wall,
    dsem, rsem, fsem,
    s1s, s1r, s2s, s2r, izs, izr, iys, iyr,
    gxss, gxsr, gyss, gysr, gzss, gzsr, gass, gasr,
    qdsem, qxss, qxsr, qfsem,
    wyss, wysr, wzss, wzsr, wxss, wxsr,
):
    nx, nc, nz, ny, iters = dims
    nxc, npair, nblk = nx * nc, nz // 2, nx - 1
    k = pt.shape[0]
    feats = pt.shape[1]
    half = feats // nc
    rank_half = f_in.shape[1]
    rows = dv.shape[0] // ny
    x, f, c = lax.axis_index("samples"), lax.axis_index("features"), lax.axis_index("rhs")
    z, y = lax.div(f, ny), lax.rem(f, ny)
    other = 1 - c
    j = c * nx + x

    def to_y(yy):
        return {"features": z * ny + yy}

    def to_z(zz):
        return {"features": zz * ny + y}

    def to_core():
        return {"rhs": other}

    def to_x(xx):
        return {"samples": xx}

    def to_j(jj):
        return {"samples": lax.rem(jj, nx), "rhs": lax.div(jj, nx)}

    def copy(src, dst, ss, rs, dev):
        return pltpu.make_async_remote_copy(
            src_ref=src, dst_ref=dst, send_sem=ss, recv_sem=rs, device_id=dev, device_id_type=MESH
        )

    def start_all(ref, me, n, to, ss, rs):
        for d in range(1, n):
            other_one = lax.rem(me + d, n)
            copy(ref.at[me], ref.at[me], ss.at[d], rs.at[me], to(other_one)).start()

    def wait_all(ref, me, n, to, ss, rs):
        for d in range(1, n):
            other_one = lax.rem(me + d, n)
            copy(ref.at[other_one], ref.at[other_one], ss.at[d], rs.at[other_one], to(other_one)).wait_recv()

    def sent_all(ref, me, n, to, ss, rs):
        for d in range(1, n):
            other_one = lax.rem(me + d, n)
            copy(ref.at[me], ref.at[me], ss.at[d], rs.at[me], to(other_one)).wait_send()

    def total(ref, n):
        t = ref[0].astype(F32)
        for i in range(1, n):
            t = t + ref[i].astype(F32)
        return t

    loads = [
        pltpu.make_async_copy(d_hbm.at[pl.ds(i * rows, rows)], dv.at[pl.ds(i * rows, rows)], dsem.at[i])
        for i in range(ny)
    ]
    for load in loads:
        load.start()

    barrier = pltpu.get_barrier_semaphore()
    for d in range(1, ny):
        pl.semaphore_signal(barrier, inc=1, device_id=to_y(lax.rem(y + d, ny)), device_id_type=MESH)
    for d in range(1, nz):
        pl.semaphore_signal(barrier, inc=1, device_id=to_z(lax.rem(z + d, nz)), device_id_type=MESH)
    for d in range(1, nxc):
        pl.semaphore_signal(barrier, inc=1, device_id=to_j(lax.rem(j + d, nxc)), device_id_type=MESH)
    pl.semaphore_wait(barrier, ny + nz + nxc - 3)

    send_r = copy(rt_in, rfull.at[c], rsem.at[0], rsem.at[1], to_core())
    send_r.start()
    send_f = copy(f_in, fall.at[c], fsem.at[0], fsem.at[1], to_core())
    send_f.start()
    rfull[c] = rt_in[...]
    fall[c] = f_in[...]

    def plane_start(value):
        wyr[y] = value.astype(WIRE)
        start_all(wyr, y, ny, to_y, wyss, wysr)

    def plane_finish():
        wait_all(wyr, y, ny, to_y, wyss, wysr)
        wzr[z] = total(wyr, ny).astype(WIRE)
        start_all(wzr, z, nz, to_z, wzss, wzsr)
        sent_all(wyr, y, ny, to_y, wyss, wysr)
        wait_all(wzr, z, nz, to_z, wzss, wzsr)
        wall[j] = total(wzr, nz).astype(WIRE)
        start_all(wall, j, nxc, to_j, wxss, wxsr)
        sent_all(wzr, z, nz, to_z, wzss, wzsr)
        wait_all(wall, j, nxc, to_j, wxss, wxsr)
        sent_all(wall, j, nxc, to_j, wxss, wxsr)

    def gathered():
        return jnp.concatenate([wall[cc * nx + b].astype(F32) for cc in range(nc) for b in range(nblk)], 1)

    def own_block(value):
        return rows_fine(value, nn, f_in[:, pl.ds(pl.multiple_of(x * LANES, LANES), LANES)])

    def spread(scaled):
        out = rows_fine(scaled[:, :rank_half], nt, fall[0])
        return out + rows_fine(scaled[:, rank_half:], nt, fall[1])

    copy(rt_in, rfull.at[other], rsem.at[0], rsem.at[1], to_core()).wait_recv()
    rt[...] = rfull[...].reshape(k, feats)
    xt[...] = jnp.zeros_like(xt)

    @pl.when(x < nblk)
    def _():
        plane_start(own_block(rt[...]))

    @pl.when(x == nblk)
    def _():
        plane_start(jnp.zeros((k, LANES), F32))

    plane_finish()
    copy(f_in, fall.at[other], fsem.at[0], fsem.at[1], to_core()).wait_recv()
    send_r.wait_send()
    send_f.wait_send()
    yt[...] = gathered()
    pt[...] = rt[...] + spread(yt[...] * shrink[...])
    for load in loads:
        load.wait()

    y_order = [d for d in (2, 1, 3) if d < ny]
    z_order = [d for d in (1, 7, 2, 6, 3, 5, 4) if d < nz]
    pair_order = [(npair // 2 + s) % npair for s in (0, 3, 1, 2)][:npair] if npair == 4 else list(range(1, npair)) + [0]
    pair_order = [p for p in pair_order if p] + [0]
    zq, zb = lax.div(z, 2), lax.rem(z, 2)
    mate = z + 1 - 2 * zb

    def s1_copy(d, p):
        return copy(s1.at[d - 1, p], r1.at[ny - d - 1, p], s1s.at[d - 1, p], s1r.at[ny - d - 1, p], to_y(lax.rem(y + d, ny)))

    def r1_copy(d, p):
        return copy(s1.at[d - 1, p], r1.at[d - 1, p], s1s.at[d - 1, p], s1r.at[d - 1, p], to_y(lax.rem(y + d, ny)))

    def s2_copy(slot, b, zz):
        return copy(s2.at[slot, b], r2.at[z], s2s.at[slot, b], s2r.at[z], to_z(zz))

    def iy_copy(d, zz, zslot):
        return copy(img.at[y, zz], img.at[y, zz], iys.at[d, zslot], iyr.at[y, zz], to_y(lax.rem(y + d, ny)))

    def iteration(step, carry):
        narrow = pt[...].astype(BF16)
        for p, off in enumerate(pair_order):
            q = lax.rem(zq + off, npair)
            for d in [*y_order, 0]:
                base = lax.rem(y + d, ny) * rows + q * (2 * LANES)
                part = nt(narrow, dv[pl.ds(pl.multiple_of(base, 2 * LANES), 2 * LANES), :])
                if d:
                    s1[d - 1, p] = part.astype(BF16)
                    s1_copy(d, p).start()
                else:
                    acc1[p] = part
        for p, off in enumerate(pair_order):
            tot = acc1[p]
            for d in range(1, ny):
                r1_copy(d, p).wait_recv()
                tot = tot + r1[d - 1, p].astype(F32)
            if off:
                q = lax.rem(zq + off, npair)
                for b in range(2):
                    s2[p, b] = tot[:, b * LANES : (b + 1) * LANES].astype(BF16)
                    s2_copy(p, b, 2 * q + b).start()
            else:
                own2[0] = tot[:, :LANES]
                own2[1] = tot[:, LANES:]
                s2[p, 0] = own2[1 - zb].astype(BF16)
                s2_copy(p, 0, mate).start()
        mine = own2[zb]
        for d in range(1, nz):
            zz = lax.rem(z + d, nz)
            copy(s2.at[0, 0], r2.at[zz], s2s.at[0, 0], s2r.at[zz], to_z(zz)).wait_recv()
            mine = mine + r2[zz].astype(F32)

        img[y, z] = mine.astype(BF16)
        for d in z_order:
            zz = lax.rem(z + d, nz)
            copy(img.at[y, z], img.at[y, z], izs.at[d], izr.at[z], to_z(zz)).start()
        for d in y_order:
            iy_copy(d, z, 0).start()

        lanes = pl.ds(pl.multiple_of(j * LANES, LANES), LANES)
        p_own, r_own = pt[:, lanes], rt[:, lanes]
        both = jnp.concatenate([mine, p_own], 1)
        gc = jnp.concatenate([nt_fine(both, both), nt_fine(r_own, p_own)], 1)
        gxs[...] = gc.reshape(gxs.shape)
        for d in range(1, nxc):
            jj = lax.rem(j + d, nxc)
            copy(gxs.at[jj], gxr.at[j], gxss.at[d], gxsr.at[j], to_j(jj)).start()
        gxr[j] = gxs[j]

        def forward(d):
            zz = lax.rem(z + d, nz)
            copy(img.at[y, zz], img.at[y, zz], izs.at[d], izr.at[zz], to_z(zz)).wait_recv()
            for e in y_order:
                iy_copy(e, zz, d).start()

        def project(yy):
            flat = jnp.concatenate([img[yy, zz] for zz in range(nz)], 1)
            return nn(flat, dv[pl.ds(pl.multiple_of(yy * rows, rows), rows), :])

        for d in z_order[:4]:
            forward(d)
        wait_all(gxr, j, nxc, to_j, gxss, gxsr)
        gyr[y] = total(gxr, nxc)
        start_all(gyr, y, ny, to_y, gyss, gysr)
        for d in z_order[4:]:
            forward(d)
        qacc[...] = project(y)
        wait_all(gyr, y, ny, to_y, gyss, gysr)
        gzr[z] = total(gyr, ny)
        start_all(gzr, z, nz, to_z, gzss, gzsr)
        for d in [e for e in (1, 3, 2) if e < ny]:
            yy = lax.rem(y + d, ny)
            for zz in range(nz):
                copy(img.at[yy, zz], img.at[yy, zz], iys.at[d, 0], iyr.at[yy, zz], to_y(yy)).wait_recv()
            qacc[...] += project(yy)

        for h in range(nc):
            qds[h] = qacc[:, h * half : (h + 1) * half]
        qd = copy(qds.at[other], qdr, qdsem.at[0], qdsem.at[1], to_core())
        qd.start()
        wait_all(gzr, z, nz, to_z, gzss, gzsr)
        gall[j] = total(gzr, nz)
        start_all(gall, j, nxc, to_j, gass, gasr)
        qd.wait_recv()
        qxr[x] = (qds[c] + qdr[...]).astype(BF16)
        start_all(qxr, x, nx, to_x, qxss, qxsr)
        wait_all(gall, j, nxc, to_j, gass, gasr)
        gc = gall[...].reshape(k, 2 * k)
        inv = inverse(gc[:, :k])
        back = nn_fine(gc[:, k:], inv)
        ginv[...] = inv
        xt[...] += nn_fine(back, pt[...])
        wait_all(qxr, x, nx, to_x, qxss, qxsr)
        qf[c] = total(qxr, nx)
        qfc = copy(qf.at[c], qf.at[c], qfsem.at[0], qfsem.at[1], to_core())
        qfc.start()
        copy(qf.at[other], qf.at[other], qfsem.at[0], qfsem.at[1], to_core()).wait_recv()
        qt[...] = jnp.concatenate([qf[h] for h in range(nc)], 1) + pt[...]
        rt[...] -= nn_fine(back, qt[...])

        @pl.when(step + 1 < iters)
        def _():
            @pl.when(x < nblk)
            def _():
                plane_start(own_block(qt[...]))

            @pl.when(x == nblk)
            def _():
                cross = nt_fine(rt[...], qt[...])
                plane_start(jnp.concatenate([cross, jnp.zeros((k, LANES - k), F32)], 1))

            plane_finish()
            image = gathered()
            proj = yt[...] - nn_fine(back, image)
            yt[...] = proj
            scaled = proj * shrink[...]
            cross = wall[nx - 1].astype(F32)[:, :k] + nt_fine(scaled, image)
            coef = nn_fine(cross, ginv[...])
            pt[...] = rt[...] + spread(scaled) - nn_fine(coef, pt[...])

        for p, off in enumerate(pair_order):
            for d in range(1, ny):
                s1_copy(d, p).wait_send()
            for b in range(2 if off else 1):
                s2_copy(p, b, mate).wait_send()
        for d in range(1, nz):
            copy(img.at[y, z], img.at[y, z], izs.at[d], izr.at[z], to_z(mate)).wait_send()
        for e in range(1, ny):
            for d in range(nz):
                iy_copy(e, z, d).wait_send()
        for d in range(1, nxc):
            jj = lax.rem(j + d, nxc)
            copy(gxs.at[jj], gxr.at[j], gxss.at[d], gxsr.at[j], to_j(jj)).wait_send()
        sent_all(gyr, y, ny, to_y, gyss, gysr)
        sent_all(gzr, z, nz, to_z, gzss, gzsr)
        sent_all(gall, j, nxc, to_j, gass, gasr)
        qd.wait_send()
        sent_all(qxr, x, nx, to_x, qxss, qxsr)
        qfc.wait_send()
        return carry

    lax.fori_loop(0, iters, iteration, 0)
    mine_rows = pl.ds(pl.multiple_of(c * (k // nc), k // nc), k // nc)
    x_out[...] = xt[mine_rows, :]
    r_out[...] = rt[mine_rows, :]


def shards(sizes, design, right_side, factor, nystrom_values):
    nx, nf, nc, ny = sizes
    nz = nf // ny
    nxc, npair = nx * nc, nz // 2
    samples, feats = design.shape
    k = right_side.shape[1] * nc
    rank_half = factor.shape[1]
    shrink = (1.0 + jnp.min(nystrom_values)) / (1.0 + nystrom_values) - 1.0
    vmem = pl.BlockSpec(memory_space=pltpu.VMEM)
    dma = pltpu.SemaphoreType.DMA
    piece = (k // nxc, 2 * k)
    half = feats // nc
    scratch = [
        pltpu.VMEM((samples, feats), BF16),
        pltpu.VMEM((nc, k // nc, feats), F32),
        pltpu.VMEM((nc, feats, rank_half), BF16),
        pltpu.VMEM((k, feats), F32),
        pltpu.VMEM((k, feats), F32),
        pltpu.VMEM((k, feats), F32),
        pltpu.VMEM((k, nc * rank_half), F32),
        pltpu.VMEM((k, k), F32),
        pltpu.VMEM((k, feats), F32),
        pltpu.VMEM((ny - 1, npair, k, 2 * LANES), BF16),
        pltpu.VMEM((ny - 1, npair, k, 2 * LANES), BF16),
        pltpu.VMEM((npair, k, 2 * LANES), F32),
        pltpu.VMEM((npair, 2, k, LANES), BF16),
        pltpu.VMEM((nz, k, LANES), BF16),
        pltpu.VMEM((2, k, LANES), F32),
        pltpu.VMEM((ny, nz, k, LANES), BF16),
        pltpu.VMEM((k, feats), F32),
        pltpu.VMEM((nxc, *piece), F32),
        pltpu.VMEM((nxc, *piece), F32),
        pltpu.VMEM((ny, *piece), F32),
        pltpu.VMEM((nz, *piece), F32),
        pltpu.VMEM((nxc, *piece), F32),
        pltpu.VMEM((nc, k, half), F32),
        pltpu.VMEM((k, half), F32),
        pltpu.VMEM((nx, k, half), BF16),
        pltpu.VMEM((nc, k, half), F32),
        pltpu.VMEM((ny, k, LANES), WIRE),
        pltpu.VMEM((nz, k, LANES), WIRE),
        pltpu.VMEM((nxc, k, LANES), WIRE),
        dma((ny,)), dma((2,)), dma((2,)),
        dma((ny - 1, npair)), dma((ny - 1, npair)), dma((npair, 2)), dma((nz,)),
        dma((nz,)), dma((nz,)), dma((ny, nz)), dma((ny, nz)),
        dma((nxc,)), dma((nxc,)), dma((ny,)), dma((ny,)), dma((nz,)), dma((nz,)), dma((nxc,)), dma((nxc,)),
        dma((2,)), dma((nx,)), dma((nx,)), dma((2,)),
        dma((ny,)), dma((ny,)), dma((nz,)), dma((nz,)), dma((nxc,)), dma((nxc,)),
    ]
    shape = jax.ShapeDtypeStruct((k // nc, feats), F32)
    sol, res = pl.pallas_call(
        functools.partial(kernel, (nx, nc, nz, ny, ITERS)),
        out_shape=(shape, shape),
        in_specs=[pl.BlockSpec(memory_space=pl.ANY), vmem, vmem, vmem],
        out_specs=(vmem, vmem),
        scratch_shapes=scratch,
        compiler_params=pltpu.CompilerParams(
            collective_id=0, has_side_effects=True, vmem_limit_bytes=56 * 2**20
        ),
        name="solve",
    )(design, right_side.T, factor, shrink[None, :])
    return sol.T, res.T


def solution(mesh):
    placed = (P(("samples", "rhs"), "features"), P("features", "rhs"), P("features", "rhs"), P())
    nx, nf, nc = (mesh.shape[a] for a in ("samples", "features", "rhs"))
    ny = max(2, nf // 8)
    return jax.shard_map(
        functools.partial(shards, (nx, nf, nc, ny)),
        mesh=mesh,
        in_specs=placed,
        out_specs=(P("features", "rhs"), P("features", "rhs")),
        check_vma=False,
    )
```

```python
import functools

import jax
import jax.numpy as jnp
from jax import lax
from jax.experimental import pallas as pl
from jax.experimental.pallas import tpu as pltpu
from jax.sharding import PartitionSpec as P

ITERS = 3
LANES = 128
MESH = pl.DeviceIdType.MESH
F32 = jnp.float32
BF16 = jnp.bfloat16


def nt(a, b):
    return lax.dot_general(a, b, (((1,), (1,)), ((), ())), preferred_element_type=F32)


def nn(a, b):
    return lax.dot_general(a, b, (((1,), (0,)), ((), ())), preferred_element_type=F32)


def halves(v):
    upper = v.astype(BF16)
    lower = (v - upper.astype(F32)).astype(BF16)
    return upper, lower


def nn_fine(a, b):
    ah, al = halves(a)
    bh, bl = halves(b)
    return nn(jnp.concatenate([ah, ah, al, al], 1), jnp.concatenate([bh, bl, bh, bl], 0))


def nt_fine(a, b):
    m, n = a.shape[0], b.shape[0]
    t = nt(jnp.concatenate(halves(a), 0), jnp.concatenate(halves(b), 0))
    return t[:m, :n] + t[:m, n:] + t[m:, :n] + t[m:, n:]


def rows_fine(a, op, b):
    m = a.shape[0]
    t = op(jnp.concatenate(halves(a), 0), b)
    return t[:m] + t[m:]


def inverse(a):
    n = a.shape[0]
    lane = lax.broadcasted_iota(jnp.int32, (1, n), 1)
    sub = lax.broadcasted_iota(jnp.int32, (n, 1), 0)
    diagonal = jnp.where(lane == sub, a, 0.0)
    scale_row = lax.rsqrt(jnp.sum(diagonal, axis=0, keepdims=True))
    scale_col = lax.rsqrt(jnp.sum(diagonal, axis=1, keepdims=True))
    a = a * scale_row * scale_col
    for i in range(0, n, 2):
        r1, r2 = a[i : i + 1, :], a[i + 1 : i + 2, :]
        c1, c2 = a[:, i : i + 1], a[:, i + 1 : i + 2]
        p, q = a[i : i + 1, i : i + 1], a[i : i + 1, i + 1 : i + 2]
        t, s = a[i + 1 : i + 2, i : i + 1], a[i + 1 : i + 2, i + 1 : i + 2]
        over = 1.0 / (p * s - q * t)
        e1 = jnp.where(lane == i, 1.0, jnp.where(lane == i + 1, 0.0, r1))
        e2 = jnp.where(lane == i + 1, 1.0, jnp.where(lane == i, 0.0, r2))
        u1 = (s * e1 - q * e2) * over
        u2 = (p * e2 - t * e1) * over
        rest = jnp.where((lane == i) | (lane == i + 1), 0.0, a) - c1 * u1 - c2 * u2
        a = jnp.where(sub == i, u1, jnp.where(sub == i + 1, u2, rest))
    return a * scale_row * scale_col


def kernel(
    dims,
    d_hbm, rt_in, f_in, values,
    out,
    dv, rfull, fall, pt, rt, xt, yt, ginv, qt,
    s1, r1, acc1, s2, r2, own2, img, qacc,
    gxs, gxr, gyr, gzr, gall,
    qds, qdr, qxr, qf,
    wys, wyr, wzr, wall, back, shrink,
    dsem, rsem, fsem,
    s1s, s1r, s2s, s2r, izs, izr, iys, iyr,
    gxss, gxsr, gyss, gysr, gzss, gzsr, gass, gasr,
    qdsem, qxss, qxsr, qfsem,
    wyss, wysr, wzss, wzsr, wxss, wxsr,
):
    nx, nc, nz, ny, iters = dims
    nxc, npair, nblk = nx * nc, nz // 2, nx - 1
    near = [(dy, dx, dc) for dy in range(ny) for dx in range(nx) for dc in range(nc) if dy + dx + dc]
    near.sort(key=lambda o: -(min(o[0], ny - o[0]) + min(o[1], nx - o[1]) + 0.1 * o[2]))
    k = pt.shape[0]
    feats = pt.shape[1]
    half = feats // nc
    rank_half = f_in.shape[1]
    rows = dv.shape[0] // ny
    x, f, c = lax.axis_index("samples"), lax.axis_index("features"), lax.axis_index("rhs")
    z, y = lax.div(f, ny), lax.rem(f, ny)
    other = 1 - c
    j = c * nx + x

    def to_y(yy):
        return {"features": z * ny + yy}

    def to_z(zz):
        return {"features": zz * ny + y}

    def to_core():
        return {"rhs": other}

    def to_x(xx):
        return {"samples": xx}

    def to_j(jj):
        return {"samples": lax.rem(jj, nx), "rhs": lax.div(jj, nx)}

    def moved(offset):
        dy, dx, dc = offset
        return lax.rem(y + dy, ny), lax.rem(x + dx, nx), lax.rem(c + dc, nc)

    def to_near(yy, xx, cc):
        return {"samples": xx, "features": z * ny + yy, "rhs": cc}

    def copy(src, dst, ss, rs, dev):
        return pltpu.make_async_remote_copy(
            src_ref=src, dst_ref=dst, send_sem=ss, recv_sem=rs, device_id=dev, device_id_type=MESH
        )

    def start_all(ref, me, n, to, ss, rs):
        for d in range(1, n):
            other_one = lax.rem(me + d, n)
            copy(ref.at[me], ref.at[me], ss.at[d], rs.at[me], to(other_one)).start()

    def wait_all(ref, me, n, to, ss, rs):
        for d in range(1, n):
            other_one = lax.rem(me + d, n)
            copy(ref.at[other_one], ref.at[other_one], ss.at[d], rs.at[other_one], to(other_one)).wait_recv()

    def sent_all(ref, me, n, to, ss, rs):
        for d in range(1, n):
            other_one = lax.rem(me + d, n)
            copy(ref.at[me], ref.at[me], ss.at[d], rs.at[me], to(other_one)).wait_send()

    def total(ref, n):
        t = ref[0].astype(F32)
        for i in range(1, n):
            t = t + ref[i].astype(F32)
        return t

    loads = [
        pltpu.make_async_copy(d_hbm.at[pl.ds(i * rows, rows)], dv.at[pl.ds(i * rows, rows)], dsem.at[i])
        for i in range(ny)
    ]
    for load in loads:
        load.start()

    barrier = pltpu.get_barrier_semaphore()
    for d in range(1, nz):
        pl.semaphore_signal(barrier, inc=1, device_id=to_z(lax.rem(z + d, nz)), device_id_type=MESH)
    for offset in near:
        pl.semaphore_signal(barrier, inc=1, device_id=to_near(*moved(offset)), device_id_type=MESH)
    pl.semaphore_wait(barrier, nz - 1 + len(near))

    send_r = copy(rt_in, rfull.at[c], rsem.at[0], rsem.at[1], to_core())
    send_r.start()
    send_f = copy(f_in, fall.at[c], fsem.at[0], fsem.at[1], to_core())
    send_f.start()
    rfull[c] = rt_in[...]
    fall[c] = f_in[...]

    quarter = k // ny

    def plane_sum(value):
        wys[...] = value.reshape(wys.shape)
        for d in range(1, ny):
            yy = lax.rem(y + d, ny)
            copy(wys.at[yy], wyr.at[y], wyss.at[d], wysr.at[y], to_y(yy)).start()
        wyr[y] = wys[y]

    def plane_exchange():
        wait_all(wyr, y, ny, to_y, wyss, wysr)
        wzr[z] = total(wyr, ny)
        start_all(wzr, z, nz, to_z, wzss, wzsr)

    def near_copy(n, offset, source):
        yy, xx, cc = moved(offset)
        if source:
            return copy(wall.at[cc * nx + xx, yy], wall.at[cc * nx + xx, yy], wxss.at[n], wxsr.at[cc * nx + xx, yy], to_near(yy, xx, cc))
        return copy(wall.at[j, y], wall.at[j, y], wxss.at[n], wxsr.at[j, y], to_near(yy, xx, cc))

    def plane_finish():
        wait_all(wzr, z, nz, to_z, wzss, wzsr)
        whole = total(wzr, nz)
        upper, lower = halves(whole)
        wall[j, y] = jnp.where((x == nblk) & (c == 1), lower.astype(F32), upper.astype(F32)).astype(BF16)
        for n, offset in enumerate(near):
            near_copy(n, offset, False).start()
        for n, offset in enumerate(near):
            near_copy(n, offset, True).wait_recv()
        for d in range(1, ny):
            yy = lax.rem(y + d, ny)
            copy(wys.at[yy], wyr.at[y], wyss.at[d], wysr.at[y], to_y(yy)).wait_send()
        sent_all(wzr, z, nz, to_z, wzss, wzsr)
        for n, offset in enumerate(near):
            near_copy(n, offset, False).wait_send()

    def block(jj):
        return wall[jj].astype(F32).reshape(k, LANES)

    def gathered():
        return jnp.concatenate([block(cc * nx + b) for cc in range(nc) for b in range(nblk)], 1)

    def own_block(value):
        return rows_fine(value, nn, f_in[:, pl.ds(pl.multiple_of(x * LANES, LANES), LANES)])

    def spread(scaled):
        out = rows_fine(scaled[:, :rank_half], nt, fall[0])
        return out + rows_fine(scaled[:, rank_half:], nt, fall[1])

    shrink[...] = (1.0 + jnp.min(values[...], axis=1, keepdims=True)) / (1.0 + values[...]) - 1.0
    copy(rt_in, rfull.at[other], rsem.at[0], rsem.at[1], to_core()).wait_recv()
    rt[...] = rfull[...].reshape(k, feats)
    xt[...] = jnp.zeros_like(xt)

    @pl.when(x < nblk)
    def _():
        plane_sum(own_block(rt[...]))

    @pl.when(x == nblk)
    def _():
        plane_sum(jnp.zeros((k, LANES), F32))

    plane_exchange()
    plane_finish()
    copy(f_in, fall.at[other], fsem.at[0], fsem.at[1], to_core()).wait_recv()
    send_r.wait_send()
    send_f.wait_send()
    yt[...] = gathered()
    pt[...] = rt[...] + spread(yt[...] * shrink[...])
    for load in loads:
        load.wait()

    y_order = [d for d in (2, 1, 3) if d < ny]
    z_order = [d for d in (1, 7, 2, 6, 3, 5, 4) if d < nz]
    pair_order = [(npair // 2 + s) % npair for s in (0, 3, 1, 2)][:npair] if npair == 4 else list(range(1, npair)) + [0]
    pair_order = [p for p in pair_order if p] + [0]
    zq, zb = lax.div(z, 2), lax.rem(z, 2)
    mate = z + 1 - 2 * zb

    def s1_copy(d, p):
        return copy(s1.at[d - 1, p], r1.at[ny - d - 1, p], s1s.at[d - 1, p], s1r.at[ny - d - 1, p], to_y(lax.rem(y + d, ny)))

    def r1_copy(d, p):
        return copy(s1.at[d - 1, p], r1.at[d - 1, p], s1s.at[d - 1, p], s1r.at[d - 1, p], to_y(lax.rem(y + d, ny)))

    def s2_copy(slot, b, zz):
        return copy(s2.at[slot, b], r2.at[z], s2s.at[slot, b], s2r.at[z], to_z(zz))

    def iy_copy(d, zz, zslot):
        return copy(img.at[y, zz], img.at[y, zz], iys.at[d, zslot], iyr.at[y, zz], to_y(lax.rem(y + d, ny)))

    def iteration(step, carry):
        narrow = pt[...].astype(BF16)
        for p, off in enumerate(pair_order):
            q = lax.rem(zq + off, npair)
            order = [*y_order, 0]
            for n in range(0, len(order), 2):
                parts = []
                for d in order[n : n + 2]:
                    base = lax.rem(y + d, ny) * rows + q * (2 * LANES)
                    parts.append(nt(narrow, dv[pl.ds(pl.multiple_of(base, 2 * LANES), 2 * LANES), :]))
                for d, part in zip(order[n : n + 2], parts):
                    if d:
                        s1[d - 1, p] = part.astype(BF16)
                    else:
                        acc1[p] = part
                for d in order[n : n + 2]:
                    if d:
                        s1_copy(d, p).start()
        for p, off in enumerate(pair_order):
            tot = acc1[p]
            for d in range(1, ny):
                r1_copy(d, p).wait_recv()
                tot = tot + r1[d - 1, p].astype(F32)
            if off:
                q = lax.rem(zq + off, npair)
                for b in range(2):
                    s2[p, b] = tot[:, b * LANES : (b + 1) * LANES].astype(BF16)
                    s2_copy(p, b, 2 * q + b).start()
            else:
                own2[0] = tot[:, :LANES]
                own2[1] = tot[:, LANES:]
                s2[p, 0] = own2[1 - zb].astype(BF16)
                s2_copy(p, 0, mate).start()
        mine = own2[zb]
        for d in range(1, nz):
            zz = lax.rem(z + d, nz)
            copy(s2.at[0, 0], r2.at[zz], s2s.at[0, 0], s2r.at[zz], to_z(zz)).wait_recv()
            mine = mine + r2[zz].astype(F32)

        img[y, z] = mine.astype(BF16)
        for d in z_order:
            zz = lax.rem(z + d, nz)
            copy(img.at[y, z], img.at[y, z], izs.at[d], izr.at[z], to_z(zz)).start()
        for d in y_order:
            iy_copy(d, z, 0).start()

        lanes = pl.ds(pl.multiple_of(j * LANES, LANES), LANES)
        p_own, r_own = pt[:, lanes], rt[:, lanes]
        both = jnp.concatenate([mine, p_own], 1)
        gc = jnp.concatenate([nt_fine(both, both), nt_fine(r_own, p_own)], 1)
        gxs[...] = gc.reshape(gxs.shape)
        for d in range(1, nxc):
            jj = lax.rem(j + d, nxc)
            copy(gxs.at[jj], gxr.at[j], gxss.at[d], gxsr.at[j], to_j(jj)).start()
        gxr[j] = gxs[j]

        def forward(d):
            zz = lax.rem(z + d, nz)
            copy(img.at[y, zz], img.at[y, zz], izs.at[d], izr.at[zz], to_z(zz)).wait_recv()
            for e in y_order:
                iy_copy(e, zz, d).start()

        def project(yy):
            flat = jnp.concatenate([img[yy, zz] for zz in range(nz)], 1)
            return nn(flat, dv[pl.ds(pl.multiple_of(yy * rows, rows), rows), :])

        for d in z_order[:4]:
            forward(d)
        wait_all(gxr, j, nxc, to_j, gxss, gxsr)
        gyr[y] = total(gxr, nxc)
        start_all(gyr, y, ny, to_y, gyss, gysr)
        for d in z_order[4:]:
            forward(d)
        qacc[...] = project(y)
        wait_all(gyr, y, ny, to_y, gyss, gysr)
        gzr[z] = total(gyr, ny)
        start_all(gzr, z, nz, to_z, gzss, gzsr)
        for d in [e for e in (1, 3, 2) if e < ny]:
            yy = lax.rem(y + d, ny)
            for zz in range(nz):
                copy(img.at[yy, zz], img.at[yy, zz], iys.at[d, 0], iyr.at[yy, zz], to_y(yy)).wait_recv()
            qacc[...] += project(yy)

        for h in range(nc):
            qds[h] = qacc[:, h * half : (h + 1) * half]
        qd = copy(qds.at[other], qdr, qdsem.at[0], qdsem.at[1], to_core())
        qd.start()
        qd.wait_recv()
        qxr[x] = (qds[c] + qdr[...]).astype(BF16)
        start_all(qxr, x, nx, to_x, qxss, qxsr)
        wait_all(gzr, z, nz, to_z, gzss, gzsr)
        gall[j] = total(gzr, nz)
        start_all(gall, j, nxc, to_j, gass, gasr)

        def step_coefficient():
            wait_all(gall, j, nxc, to_j, gass, gasr)
            gc = gall[...].reshape(k, 2 * k)
            inv = inverse(gc[:, :k])
            ginv[...] = inv
            back[...] = nn_fine(gc[:, k:], inv)
            xt[...] += nn_fine(back[...], pt[...])

        @pl.when(step + 1 == iters)
        def _():
            step_coefficient()

        wait_all(qxr, x, nx, to_x, qxss, qxsr)
        qf[c] = total(qxr, nx)
        qfc = copy(qf.at[c], qf.at[c], qfsem.at[0], qfsem.at[1], to_core())
        qfc.start()
        copy(qf.at[other], qf.at[other], qfsem.at[0], qfsem.at[1], to_core()).wait_recv()
        qt[...] = jnp.concatenate([qf[h] for h in range(nc)], 1) + pt[...]

        @pl.when(step + 1 == iters)
        def _():
            rt[...] -= nn_fine(back[...], qt[...])

        @pl.when(step + 1 < iters)
        def _():
            @pl.when(x < nblk)
            def _():
                plane_sum(own_block(qt[...]))

            @pl.when(x == nblk)
            def _():
                plane_sum(jnp.concatenate([nt_fine(rt[...], qt[...]), nt_fine(qt[...], qt[...])], 1))

            plane_exchange()
            step_coefficient()
            rt[...] -= nn_fine(back[...], qt[...])
            plane_finish()
            image = gathered()
            small = block(nx - 1) + block(nx * nc - 1)
            proj = yt[...] - nn_fine(back[...], image)
            yt[...] = proj
            scaled = proj * shrink[...]
            cross = small[:, :k] - nn_fine(back[...], small[:, k:]) + nt_fine(scaled, image)
            coef = nn_fine(cross, ginv[...])
            pt[...] = rt[...] + spread(scaled) - nn_fine(coef, pt[...])

        for p, off in enumerate(pair_order):
            for d in range(1, ny):
                s1_copy(d, p).wait_send()
            for b in range(2 if off else 1):
                s2_copy(p, b, mate).wait_send()
        for d in range(1, nz):
            copy(img.at[y, z], img.at[y, z], izs.at[d], izr.at[z], to_z(mate)).wait_send()
        for e in range(1, ny):
            for d in range(nz):
                iy_copy(e, z, d).wait_send()
        for d in range(1, nxc):
            jj = lax.rem(j + d, nxc)
            copy(gxs.at[jj], gxr.at[j], gxss.at[d], gxsr.at[j], to_j(jj)).wait_send()
        sent_all(gyr, y, ny, to_y, gyss, gysr)
        sent_all(gzr, z, nz, to_z, gzss, gzsr)
        sent_all(gall, j, nxc, to_j, gass, gasr)
        qd.wait_send()
        sent_all(qxr, x, nx, to_x, qxss, qxsr)
        qfc.wait_send()
        return carry

    lax.fori_loop(0, iters, iteration, 0)
    mine_rows = pl.ds(pl.multiple_of(c * (k // nc), k // nc), k // nc)
    out[0] = xt[mine_rows, :]
    out[1] = rt[mine_rows, :]


def shards(sizes, design, right_side, factor, nystrom_values):
    nx, nf, nc, ny = sizes
    nz = nf // ny
    nxc, npair = nx * nc, nz // 2
    samples, feats = design.shape
    k = right_side.shape[1] * nc
    rank_half = factor.shape[1]
    vmem = pl.BlockSpec(memory_space=pltpu.VMEM)
    dma = pltpu.SemaphoreType.DMA
    piece = (k // nxc, 2 * k)
    half = feats // nc
    scratch = [
        pltpu.VMEM((samples, feats), BF16),
        pltpu.VMEM((nc, k // nc, feats), F32),
        pltpu.VMEM((nc, feats, rank_half), BF16),
        pltpu.VMEM((k, feats), F32),
        pltpu.VMEM((k, feats), F32),
        pltpu.VMEM((k, feats), F32),
        pltpu.VMEM((k, nc * rank_half), F32),
        pltpu.VMEM((k, k), F32),
        pltpu.VMEM((k, feats), F32),
        pltpu.VMEM((ny - 1, npair, k, 2 * LANES), BF16),
        pltpu.VMEM((ny - 1, npair, k, 2 * LANES), BF16),
        pltpu.VMEM((npair, k, 2 * LANES), F32),
        pltpu.VMEM((npair, 2, k, LANES), BF16),
        pltpu.VMEM((nz, k, LANES), BF16),
        pltpu.VMEM((2, k, LANES), F32),
        pltpu.VMEM((ny, nz, k, LANES), BF16),
        pltpu.VMEM((k, feats), F32),
        pltpu.VMEM((nxc, *piece), F32),
        pltpu.VMEM((nxc, *piece), F32),
        pltpu.VMEM((ny, *piece), F32),
        pltpu.VMEM((nz, *piece), F32),
        pltpu.VMEM((nxc, *piece), F32),
        pltpu.VMEM((nc, k, half), F32),
        pltpu.VMEM((k, half), F32),
        pltpu.VMEM((nx, k, half), BF16),
        pltpu.VMEM((nc, k, half), F32),
        pltpu.VMEM((ny, k // ny, LANES), F32),
        pltpu.VMEM((ny, k // ny, LANES), F32),
        pltpu.VMEM((nz, k // ny, LANES), F32),
        pltpu.VMEM((nxc, ny, k // ny, LANES), BF16),
        pltpu.VMEM((k, k), F32),
        pltpu.VMEM((1, nc * rank_half), F32),
        dma((ny,)), dma((2,)), dma((2,)),
        dma((ny - 1, npair)), dma((ny - 1, npair)), dma((npair, 2)), dma((nz,)),
        dma((nz,)), dma((nz,)), dma((ny, nz)), dma((ny, nz)),
        dma((nxc,)), dma((nxc,)), dma((ny,)), dma((ny,)), dma((nz,)), dma((nz,)), dma((nxc,)), dma((nxc,)),
        dma((2,)), dma((nx,)), dma((nx,)), dma((2,)),
        dma((ny,)), dma((ny,)), dma((nz,)), dma((nz,)), dma((nxc * ny,)), dma((nxc, ny)),
    ]
    out = pl.pallas_call(
        functools.partial(kernel, (nx, nc, nz, ny, ITERS)),
        out_shape=jax.ShapeDtypeStruct((2, k // nc, feats), F32),
        in_specs=[pl.BlockSpec(memory_space=pl.ANY), vmem, vmem, vmem],
        out_specs=vmem,
        scratch_shapes=scratch,
        compiler_params=pltpu.CompilerParams(
            collective_id=0, has_side_effects=True, vmem_limit_bytes=56 * 2**20
        ),
        name="solve",
    )(design, right_side.T, factor, nystrom_values[None, :])
    return out[0].T, out[1].T


def solution(mesh):
    placed = (P(("samples", "rhs"), "features"), P("features", "rhs"), P("features", "rhs"), P())
    nx, nf, nc = (mesh.shape[a] for a in ("samples", "features", "rhs"))
    ny = max(2, nf // 8)
    return jax.shard_map(
        functools.partial(shards, (nx, nf, nc, ny)),
        mesh=mesh,
        in_specs=placed,
        out_specs=(P("features", "rhs"), P("features", "rhs")),
        check_vma=False,
    )
```

```python
import functools

import jax
import jax.numpy as jnp
from jax import lax
from jax.experimental import pallas as pl
from jax.experimental.pallas import tpu as pltpu
from jax.sharding import PartitionSpec as P

ITERS = 3
LANES = 128
MESH = pl.DeviceIdType.MESH
F32 = jnp.float32
BF16 = jnp.bfloat16


def nt(a, b):
    return lax.dot_general(a, b, (((1,), (1,)), ((), ())), preferred_element_type=F32)


def nn(a, b):
    return lax.dot_general(a, b, (((1,), (0,)), ((), ())), preferred_element_type=F32)


def halves(v):
    upper = v.astype(BF16)
    lower = (v - upper.astype(F32)).astype(BF16)
    return upper, lower


def wide(a):
    upper, lower = halves(a)
    return jnp.concatenate([upper, upper, lower, lower], 1)


def tall(b):
    return jnp.concatenate(halves(b) * 2, 0)


def nn_fine(a, b):
    return nn(wide(a), tall(b))


def nt_fine(a, b):
    m, n = a.shape[0], b.shape[0]
    t = nt(jnp.concatenate(halves(a), 0), jnp.concatenate(halves(b), 0))
    return t[:m, :n] + t[:m, n:] + t[m:, :n] + t[m:, n:]


def rows_fine(a, op, b):
    m = a.shape[0]
    t = op(jnp.concatenate(halves(a), 0), b)
    return t[:m] + t[m:]


def inverse(a, width=8):
    n = a.shape[0]
    lane = lax.broadcasted_iota(jnp.int32, (1, n), 1)
    sub = lax.broadcasted_iota(jnp.int32, (n, 1), 0)
    for i in range(0, n, width):
        cols = [jnp.broadcast_to(a[:, i + t : i + t + 1], (n, n)) for t in range(width)]
        pivots = [[cols[t][i + r : i + r + 1, :] for t in range(width)] for r in range(width)]
        inside = (lane >= i) & (lane < i + width)
        rows = [jnp.where(lane == i + r, 1.0, jnp.where(inside, 0.0, a[i + r : i + r + 1, :])) for r in range(width)]
        for r in range(width):
            over = 1.0 / pivots[r][r]
            rows[r] = rows[r] * over
            for t in range(r + 1, width):
                pivots[r][t] = pivots[r][t] * over
            for q in range(width):
                if q != r:
                    factor = pivots[q][r]
                    rows[q] = rows[q] - factor * rows[r]
                    for t in range(r + 1, width):
                        pivots[q][t] = pivots[q][t] - factor * pivots[r][t]
        a = jnp.where(inside, 0.0, a)
        for r in range(width):
            a = a - cols[r] * rows[r]
        for r in range(width):
            a = jnp.where(sub == i + r, rows[r], a)
    return a


def kernel(
    dims,
    d_hbm, rt_in, f_in, values,
    out,
    dv, rfull, fall, pt, rt, xt, yt, gp, qt,
    s0, r0, s1, r1, acc0, acc1, s2, r2, img, qacc,
    gxs, gxr, gyr, gzr, gall,
    qds, qdr, qxr, qf,
    wys, wyr, wzr, wall, back, shrink,
    dsem, rsem, fsem,
    s0s, s0r, s1s, s1r, s2s, s2r, izs, izr, iys, iyr, ifs,
    gxss, gxsr, gyss, gysr, gzss, gzsr, gass, gasr,
    qdsem, qxss, qxsr, qfsem,
    wyss, wysr, wzss, wzsr, wxss, wxsr,
):
    nx, nc, nz, ny, iters = dims
    nxc, nblk = nx * nc, nx - 1
    near = [(dy, dx, dc) for dy in range(ny) for dx in range(nx) for dc in range(nc) if dy + dx + dc]
    near.sort(key=lambda o: -(min(o[0], ny - o[0]) + min(o[1], nx - o[1]) + 0.1 * o[2]))
    k = pt.shape[0]
    feats = pt.shape[1]
    half = feats // nc
    rank_half = f_in.shape[1]
    rows = dv.shape[0] // ny
    x, f, c = lax.axis_index("samples"), lax.axis_index("features"), lax.axis_index("rhs")
    z, y = lax.div(f, ny), lax.rem(f, ny)
    other = 1 - c
    j = c * nx + x

    def to_y(yy):
        return {"features": z * ny + yy}

    def to_z(zz):
        return {"features": zz * ny + y}

    def to_core():
        return {"rhs": other}

    def to_x(xx):
        return {"samples": xx}

    def to_j(jj):
        return {"samples": lax.rem(jj, nx), "rhs": lax.div(jj, nx)}

    def moved(offset):
        dy, dx, dc = offset
        return lax.rem(y + dy, ny), lax.rem(x + dx, nx), lax.rem(c + dc, nc)

    def to_near(yy, xx, cc):
        return {"samples": xx, "features": z * ny + yy, "rhs": cc}

    def copy(src, dst, ss, rs, dev):
        return pltpu.make_async_remote_copy(
            src_ref=src, dst_ref=dst, send_sem=ss, recv_sem=rs, device_id=dev, device_id_type=MESH
        )

    def start_all(ref, me, n, to, ss, rs):
        for d in range(1, n):
            other_one = lax.rem(me + d, n)
            copy(ref.at[me], ref.at[me], ss.at[d], rs.at[me], to(other_one)).start()

    def wait_all(ref, me, n, to, ss, rs):
        for d in range(1, n):
            other_one = lax.rem(me + d, n)
            copy(ref.at[other_one], ref.at[other_one], ss.at[d], rs.at[other_one], to(other_one)).wait_recv()

    def sent_all(ref, me, n, to, ss, rs):
        for d in range(1, n):
            other_one = lax.rem(me + d, n)
            copy(ref.at[me], ref.at[me], ss.at[d], rs.at[me], to(other_one)).wait_send()

    def total(ref, n):
        t = ref[0].astype(F32)
        for i in range(1, n):
            t = t + ref[i].astype(F32)
        return t

    loads = [
        pltpu.make_async_copy(d_hbm.at[pl.ds(i * rows, rows)], dv.at[pl.ds(i * rows, rows)], dsem.at[i])
        for i in range(ny)
    ]
    load_r = pltpu.make_async_copy(rt_in, rfull.at[c], dsem.at[ny])
    load_f = pltpu.make_async_copy(f_in, fall.at[c], dsem.at[ny + 1])
    load_r.start()
    load_f.start()
    for load in loads:
        load.start()

    barrier = pltpu.get_barrier_semaphore()
    for d in range(1, nz):
        pl.semaphore_signal(barrier, inc=1, device_id=to_z(lax.rem(z + d, nz)), device_id_type=MESH)
    for offset in near:
        pl.semaphore_signal(barrier, inc=1, device_id=to_near(*moved(offset)), device_id_type=MESH)
    pl.semaphore_wait(barrier, nz - 1 + len(near))

    load_r.wait()
    send_r = copy(rfull.at[c], rfull.at[c], rsem.at[0], rsem.at[1], to_core())
    send_r.start()
    load_f.wait()
    send_f = copy(fall.at[c], fall.at[c], fsem.at[0], fsem.at[1], to_core())
    send_f.start()

    quarter = k // ny

    def plane_sum(value):
        wys[...] = value.reshape(wys.shape)
        for d in range(1, ny):
            yy = lax.rem(y + d, ny)
            copy(wys.at[yy], wyr.at[y], wyss.at[d], wysr.at[y], to_y(yy)).start()
        wyr[y] = wys[y]

    def plane_exchange():
        wait_all(wyr, y, ny, to_y, wyss, wysr)
        wzr[z] = total(wyr, ny)
        start_all(wzr, z, nz, to_z, wzss, wzsr)

    def near_copy(n, offset, source):
        yy, xx, cc = moved(offset)
        if source:
            return copy(wall.at[cc * nx + xx, yy], wall.at[cc * nx + xx, yy], wxss.at[n], wxsr.at[cc * nx + xx, yy], to_near(yy, xx, cc))
        return copy(wall.at[j, y], wall.at[j, y], wxss.at[n], wxsr.at[j, y], to_near(yy, xx, cc))

    def plane_finish():
        wait_all(wzr, z, nz, to_z, wzss, wzsr)
        whole = total(wzr, nz)
        upper, lower = halves(whole)
        wall[j, y] = jnp.where((x == nblk) & (c == 1), lower.astype(F32), upper.astype(F32)).astype(BF16)
        for n, offset in enumerate(near):
            near_copy(n, offset, False).start()
        for n, offset in enumerate(near):
            near_copy(n, offset, True).wait_recv()
        for d in range(1, ny):
            yy = lax.rem(y + d, ny)
            copy(wys.at[yy], wyr.at[y], wyss.at[d], wysr.at[y], to_y(yy)).wait_send()
        sent_all(wzr, z, nz, to_z, wzss, wzsr)
        for n, offset in enumerate(near):
            near_copy(n, offset, False).wait_send()

    def block(jj):
        return wall[jj].reshape(k, LANES)

    def gathered():
        return jnp.concatenate([block(cc * nx + b) for cc in range(nc) for b in range(nblk)], 1)

    def own_block(value):
        return rows_fine(value, nn, fall[c, :, pl.ds(pl.multiple_of(x * LANES, LANES), LANES)])

    def spread(scaled):
        out = rows_fine(scaled[:, :rank_half], nt, fall[0])
        return out + rows_fine(scaled[:, rank_half:], nt, fall[1])

    least = jnp.min(jnp.min(values[...], axis=1, keepdims=True), axis=0, keepdims=True)
    table = (1.0 + least) / (1.0 + values[...]) - 1.0
    for r in range(values.shape[0]):
        shrink[:, r * LANES : (r + 1) * LANES] = table[r : r + 1, :]
    copy(rfull.at[c], rfull.at[other], rsem.at[0], rsem.at[1], to_core()).wait_recv()
    rt[...] = rfull[...].reshape(k, feats)
    xt[...] = jnp.zeros_like(xt)

    @pl.when(x < nblk)
    def _():
        plane_sum(own_block(rt[...]))

    @pl.when(x == nblk)
    def _():
        plane_sum(jnp.zeros((k, LANES), F32))

    plane_exchange()
    plane_finish()
    copy(fall.at[c], fall.at[other], fsem.at[0], fsem.at[1], to_core()).wait_recv()
    send_r.wait_send()
    send_f.wait_send()
    yt[...] = gathered().astype(F32)
    pt[...] = rt[...] + spread(yt[...] * shrink[...])
    for load in loads:
        load.wait()

    y_order = [d for d in (2, 1, 3) if d < ny]
    beside = (1, nz - 1)
    distant = sorted(range(2, nz - 1), key=lambda d: -min(d, nz - d))
    arriving = distant[::-1]
    pieces = [*distant, 0]
    pairs = [(n, pieces[n : n + 2]) for n in range(0, len(pieces), 2)]

    def along_z(d):
        return lax.rem(z + d, nz)

    def along_y(d):
        return lax.rem(y + d, ny)

    def products(narrow, parts, offsets):
        start = [pl.multiple_of(along_y(d) * rows + along_z(o) * LANES, LANES) for d in parts for o in offsets]
        part = nt(narrow, jnp.concatenate([dv[pl.ds(at, LANES), :] for at in start], 0))
        cut = [part[:, n * LANES : (n + 1) * LANES] for n in range(len(start))]
        return [(d, cut[n * len(offsets) : (n + 1) * len(offsets)]) for n, d in enumerate(parts)]

    def s0_copy(b, d):
        return copy(s0.at[b, d], r0.at[b, d], s0s.at[b, d], s0r.at[b, d], to_z(along_z(beside[b])))

    def s1_copy(d, n, count, received=False):
        at = pl.ds(n, count)
        back_slot = d - 1 if received else ny - d - 1
        return copy(s1.at[d - 1, at], r1.at[back_slot, at], s1s.at[d - 1, n], s1r.at[back_slot, n], to_y(along_y(d)))

    def s2_copy(n, d):
        return copy(s2.at[n], r2.at[z], s2s.at[n], s2r.at[z], to_z(along_z(d)))

    def iy_copy(d, zz, slot):
        return copy(img.at[y, zz], img.at[y, zz], iys.at[d, slot], iyr.at[y, zz], to_y(along_y(d)))

    def if_copy(b, d):
        yy = along_y(d)
        return copy(img.at[yy, z], img.at[yy, z], ifs.at[b, d], iyr.at[yy, z], to_z(along_z(beside[b])))

    def iteration(step, carry):
        narrow = pt[...].astype(BF16)
        order = [*y_order, 0]
        parts = [order[n : n + 2] for n in range(0, ny, 2)]

        def beside_products(some):
            made = products(narrow, some, beside)
            for d, cut in made:
                for b in range(2):
                    s0[b, d] = cut[b].astype(BF16)
            for d, _ in made:
                for b in range(2):
                    s0_copy(b, d).start()

        def y_products(some, n, offsets):
            sent = [o for o in offsets if o]
            made = products(narrow, some, offsets)
            for d, cut in made:
                for m, part in enumerate(cut):
                    if not d:
                        acc1[n + m] = part
                    elif offsets[m]:
                        s1[d - 1, n + m] = part.astype(BF16)
                    else:
                        acc0[d] = part
            for d, _ in made:
                if d and sent:
                    s1_copy(d, n, len(sent)).start()

        for some in parts:
            y_products(some, *pairs[0])
            beside_products(some)
        for n, offsets in pairs[1:]:
            for some in parts:
                y_products(some, n, offsets)
        last = len(distant)
        for d in [*y_order, 0]:
            for b in range(2):
                s0_copy(b, d).wait_recv()
            from_sides = r0[0, d].astype(F32) + r0[1, d].astype(F32)
            if d:
                s1[d - 1, last] = (acc0[d] + from_sides).astype(BF16)
                s1_copy(d, last, 1).start()
            else:
                acc1[last] += from_sides
        for n, offsets in pairs:
            sent = [o for o in offsets if o]
            if sent:
                for d in range(1, ny):
                    s1_copy(d, n, len(sent), True).wait_recv()
            for m, o in enumerate(sent):
                tot = acc1[n + m]
                for d in range(1, ny):
                    tot = tot + r1[d - 1, n + m].astype(F32)
                s2[n + m] = tot.astype(BF16)
            for m, o in enumerate(sent):
                s2_copy(n + m, o).start()
        mine = acc1[last]
        for d in range(1, ny):
            s1_copy(d, last, 1, True).wait_recv()
            mine = mine + r1[d - 1, last].astype(F32)
        for d in arriving[::-1]:
            zz = along_z(d)
            copy(s2.at[0], r2.at[zz], s2s.at[0], s2r.at[zz], to_z(zz)).wait_recv()
            mine = mine + r2[zz].astype(F32)

        img[y, z] = mine.astype(BF16)
        for d in y_order:
            iy_copy(d, z, 0).start()
        for d in [*distant, *beside]:
            copy(img.at[y, z], img.at[y, z], izs.at[d], izr.at[z], to_z(along_z(d))).start()

        lanes = pl.ds(pl.multiple_of(j * LANES, LANES), LANES)
        p_own, r_own = pt[:, lanes], rt[:, lanes]
        both = jnp.concatenate([mine, p_own], 1)
        gc = jnp.concatenate([nt_fine(both, both), nt_fine(r_own, p_own)], 1)
        gxs[...] = gc.reshape(gxs.shape)
        for d in range(1, nxc):
            jj = lax.rem(j + d, nxc)
            copy(gxs.at[jj], gxr.at[j], gxss.at[d], gxsr.at[j], to_j(jj)).start()
        gxr[j] = gxs[j]

        def arrived(d):
            zz = along_z(d)
            copy(img.at[y, zz], img.at[y, zz], izs.at[d], izr.at[zz], to_z(zz)).wait_recv()

        def forward(d):
            arrived(d)
            for e in y_order:
                iy_copy(e, along_z(d), d).start()

        def y_arrived(d, zz):
            yy = along_y(d)
            copy(img.at[yy, zz], img.at[yy, zz], iys.at[d, 0], iyr.at[yy, zz], to_y(yy)).wait_recv()

        def project(yy):
            flat = jnp.concatenate([img[yy, zz] for zz in range(nz)], 1)
            return nn(flat, dv[pl.ds(pl.multiple_of(yy * rows, rows), rows), :])

        for d in y_order[::-1]:
            y_arrived(d, z)
            for b in range(2):
                if_copy(b, d).start()
        for d in arriving[:2]:
            forward(d)
        for d in arriving[2:]:
            forward(d)
        wait_all(gxr, j, nxc, to_j, gxss, gxsr)
        gyr[y] = total(gxr, nxc)
        start_all(gyr, y, ny, to_y, gyss, gysr)
        for d in beside:
            arrived(d)
        qacc[...] = project(y)
        for d in [e for e in (1, 3, 2) if e < ny]:
            if d == y_order[0]:
                wait_all(gyr, y, ny, to_y, gyss, gysr)
                gzr[z] = total(gyr, ny)
                start_all(gzr, z, nz, to_z, gzss, gzsr)
            for o in range(1, nz):
                y_arrived(d, along_z(o))
            qacc[...] += project(along_y(d))

        for h in range(nc):
            qds[h] = qacc[:, h * half : (h + 1) * half]
        qd = copy(qds.at[other], qdr, qdsem.at[0], qdsem.at[1], to_core())
        qd.start()
        qd.wait_recv()
        qxr[x] = (qds[c] + qdr[...]).astype(BF16)
        start_all(qxr, x, nx, to_x, qxss, qxsr)
        wait_all(gzr, z, nz, to_z, gzss, gzsr)
        gall[j] = total(gzr, nz)
        start_all(gall, j, nxc, to_j, gass, gasr)

        def step_coefficient():
            wait_all(gall, j, nxc, to_j, gass, gasr)
            gc = gall[...].reshape(k, 2 * k)
            inv = inverse(gc[:, :k])
            back[...] = nn_fine(gc[:, k:], inv)
            old = tall(pt[...])
            xt[...] += nn(wide(back[...]), old)
            gp[...] = tall(nn(wide(inv), old))

        @pl.when(step + 1 == iters)
        def _():
            step_coefficient()

        wait_all(qxr, x, nx, to_x, qxss, qxsr)
        qf[c] = total(qxr, nx)
        qfc = copy(qf.at[c], qf.at[c], qfsem.at[0], qfsem.at[1], to_core())
        qfc.start()
        copy(qf.at[other], qf.at[other], qfsem.at[0], qfsem.at[1], to_core()).wait_recv()
        qt[...] = jnp.concatenate([qf[h] for h in range(nc)], 1) + pt[...]

        @pl.when(step + 1 == iters)
        def _():
            rt[...] -= nn_fine(back[...], qt[...])

        @pl.when(step + 1 < iters)
        def _():
            @pl.when(x < nblk)
            def _():
                plane_sum(own_block(qt[...]))

            @pl.when(x == nblk)
            def _():
                plane_sum(jnp.concatenate([nt_fine(rt[...], qt[...]), nt_fine(qt[...], qt[...])], 1))

            plane_exchange()
            step_coefficient()
            rt[...] -= nn_fine(back[...], qt[...])
            plane_finish()
            image = gathered()
            small = block(nx - 1).astype(F32) + block(nx * nc - 1).astype(F32)
            weighted = image.astype(F32) * shrink[...]
            inner = nt(jnp.concatenate([*halves(yt[...] * shrink[...]), *halves(weighted)], 0), image)
            proj = yt[...] - rows_fine(back[...], nn, image)
            yt[...] = proj
            grown = small[:, k:] + inner[2 * k : 3 * k] + inner[3 * k :]
            cross = small[:, :k] + inner[:k] + inner[k : 2 * k] - nn_fine(back[...], grown)
            pt[...] = rt[...] + spread(proj * shrink[...]) - nn(wide(cross), gp[...])

        for d in range(ny):
            for b in range(2):
                s0_copy(b, d).wait_send()
        for n, offsets in pairs:
            sent = [o for o in offsets if o]
            for d in range(1, ny):
                if sent:
                    s1_copy(d, n, len(sent)).wait_send()
            for m, o in enumerate(sent):
                s2_copy(n + m, o).wait_send()
        for d in range(1, ny):
            s1_copy(d, last, 1).wait_send()
            for b in range(2):
                if_copy(b, d).wait_send()
            for slot in [0, *distant]:
                iy_copy(d, z, slot).wait_send()
        for d in range(1, nz):
            copy(img.at[y, z], img.at[y, z], izs.at[d], izr.at[z], to_z(along_z(d))).wait_send()
        for d in range(1, nxc):
            jj = lax.rem(j + d, nxc)
            copy(gxs.at[jj], gxr.at[j], gxss.at[d], gxsr.at[j], to_j(jj)).wait_send()
        sent_all(gyr, y, ny, to_y, gyss, gysr)
        sent_all(gzr, z, nz, to_z, gzss, gzsr)
        sent_all(gall, j, nxc, to_j, gass, gasr)
        qd.wait_send()
        sent_all(qxr, x, nx, to_x, qxss, qxsr)
        qfc.wait_send()
        return carry

    lax.fori_loop(0, iters, iteration, 0)
    mine_rows = pl.ds(pl.multiple_of(c * (k // nc), k // nc), k // nc)
    out[0] = xt[mine_rows, :]
    out[1] = rt[mine_rows, :]


def shards(sizes, design, right_side, factor, nystrom_values):
    nx, nf, nc, ny = sizes
    nz = nf // ny
    nxc = nx * nc
    samples, feats = design.shape
    k = right_side.shape[1] * nc
    rank_half = factor.shape[1]
    vmem = pl.BlockSpec(memory_space=pltpu.VMEM)
    anywhere = pl.BlockSpec(memory_space=pl.ANY)
    dma = pltpu.SemaphoreType.DMA
    piece = (k // nxc, 2 * k)
    half = feats // nc
    scratch = [
        pltpu.VMEM((samples, feats), BF16),
        pltpu.VMEM((nc, k // nc, feats), F32),
        pltpu.VMEM((nc, feats, rank_half), BF16),
        pltpu.VMEM((k, feats), F32),
        pltpu.VMEM((k, feats), F32),
        pltpu.VMEM((k, feats), F32),
        pltpu.VMEM((k, nc * rank_half), F32),
        pltpu.VMEM((4 * k, feats), BF16),
        pltpu.VMEM((k, feats), F32),
        pltpu.VMEM((2, ny, k, LANES), BF16),
        pltpu.VMEM((2, ny, k, LANES), BF16),
        pltpu.VMEM((ny - 1, nz - 2, k, LANES), BF16),
        pltpu.VMEM((ny - 1, nz - 2, k, LANES), BF16),
        pltpu.VMEM((ny, k, LANES), F32),
        pltpu.VMEM((nz - 2, k, LANES), F32),
        pltpu.VMEM((nz - 3, k, LANES), BF16),
        pltpu.VMEM((nz, k, LANES), BF16),
        pltpu.VMEM((ny, nz, k, LANES), BF16),
        pltpu.VMEM((k, feats), F32),
        pltpu.VMEM((nxc, *piece), F32),
        pltpu.VMEM((nxc, *piece), F32),
        pltpu.VMEM((ny, *piece), F32),
        pltpu.VMEM((nz, *piece), F32),
        pltpu.VMEM((nxc, *piece), F32),
        pltpu.VMEM((nc, k, half), F32),
        pltpu.VMEM((k, half), F32),
        pltpu.VMEM((nx, k, half), BF16),
        pltpu.VMEM((nc, k, half), F32),
        pltpu.VMEM((ny, k // ny, LANES), F32),
        pltpu.VMEM((ny, k // ny, LANES), F32),
        pltpu.VMEM((nz, k // ny, LANES), F32),
        pltpu.VMEM((nxc, ny, k // ny, LANES), BF16),
        pltpu.VMEM((k, k), F32),
        pltpu.VMEM((1, nc * rank_half), F32),
        dma((ny + 2,)), dma((2,)), dma((2,)),
        dma((2, ny)), dma((2, ny)), dma((ny - 1, nz)), dma((ny - 1, nz)), dma((nz,)), dma((nz,)),
        dma((nz,)), dma((nz,)), dma((ny, nz)), dma((ny, nz)), dma((2, ny)),
        dma((nxc,)), dma((nxc,)), dma((ny,)), dma((ny,)), dma((nz,)), dma((nz,)), dma((nxc,)), dma((nxc,)),
        dma((2,)), dma((nx,)), dma((nx,)), dma((2,)),
        dma((ny,)), dma((ny,)), dma((nz,)), dma((nz,)), dma((nxc * ny,)), dma((nxc, ny)),
    ]
    out = pl.pallas_call(
        functools.partial(kernel, (nx, nc, nz, ny, ITERS)),
        out_shape=jax.ShapeDtypeStruct((2, k // nc, feats), F32),
        in_specs=[anywhere, anywhere, anywhere, vmem],
        out_specs=vmem,
        scratch_shapes=scratch,
        compiler_params=pltpu.CompilerParams(
            collective_id=0, has_side_effects=True, vmem_limit_bytes=56 * 2**20
        ),
        name="solve",
    )(design, right_side.T, factor, nystrom_values.reshape(-1, LANES))
    return out[0].T, out[1].T


def solution(mesh):
    placed = (P(("samples", "rhs"), "features"), P("features", "rhs"), P("features", "rhs"), P())
    nx, nf, nc = (mesh.shape[a] for a in ("samples", "features", "rhs"))
    ny = max(2, nf // 8)
    return jax.shard_map(
        functools.partial(shards, (nx, nf, nc, ny)),
        mesh=mesh,
        in_specs=placed,
        out_specs=(P("features", "rhs"), P("features", "rhs")),
        check_vma=False,
    )
```

```python
import functools

import jax
import jax.numpy as jnp
from jax import lax
from jax.experimental import pallas as pl
from jax.experimental.pallas import tpu as pltpu
from jax.sharding import PartitionSpec as P

ITERS = 3
LANES = 128
MESH = pl.DeviceIdType.MESH
F32 = jnp.float32
BF16 = jnp.bfloat16


def nt(a, b):
    return lax.dot_general(a, b, (((1,), (1,)), ((), ())), preferred_element_type=F32)


def nn(a, b):
    return lax.dot_general(a, b, (((1,), (0,)), ((), ())), preferred_element_type=F32)


def halves(v):
    upper = v.astype(BF16)
    lower = (v - upper.astype(F32)).astype(BF16)
    return upper, lower


def wide(a):
    upper, lower = halves(a)
    return jnp.concatenate([upper, upper, lower, lower], 1)


def tall(b):
    return jnp.concatenate(halves(b) * 2, 0)


def nn_fine(a, b):
    return nn(wide(a), tall(b))


def nt_fine(a, b):
    m, n = a.shape[0], b.shape[0]
    t = nt(jnp.concatenate(halves(a), 0), jnp.concatenate(halves(b), 0))
    return t[:m, :n] + t[:m, n:] + t[m:, :n] + t[m:, n:]


def rows_fine(a, op, b):
    m = a.shape[0]
    t = op(jnp.concatenate(halves(a), 0), b)
    return t[:m] + t[m:]


def inverse(a, width=8):
    n = a.shape[0]
    lane = lax.broadcasted_iota(jnp.int32, (1, n), 1)
    sub = lax.broadcasted_iota(jnp.int32, (n, 1), 0)
    for i in range(0, n, width):
        cols = [jnp.broadcast_to(a[:, i + t : i + t + 1], (n, n)) for t in range(width)]
        pivots = [[cols[t][i + r : i + r + 1, :] for t in range(width)] for r in range(width)]
        inside = (lane >= i) & (lane < i + width)
        rows = [jnp.where(lane == i + r, 1.0, jnp.where(inside, 0.0, a[i + r : i + r + 1, :])) for r in range(width)]
        for r in range(width):
            over = 1.0 / pivots[r][r]
            rows[r] = rows[r] * over
            for t in range(r + 1, width):
                pivots[r][t] = pivots[r][t] * over
            for q in range(width):
                if q != r:
                    factor = pivots[q][r]
                    rows[q] = rows[q] - factor * rows[r]
                    for t in range(r + 1, width):
                        pivots[q][t] = pivots[q][t] - factor * pivots[r][t]
        a = jnp.where(inside, 0.0, a)
        for r in range(width):
            a = a - cols[r] * rows[r]
        for r in range(width):
            a = jnp.where(sub == i + r, rows[r], a)
    return a


def kernel(
    dims,
    d_hbm, rt_in, f_in, values,
    out,
    dv, rfull, fall, pt, rt, xt, yt, gp, qt,
    s0, r0, s1, r1, acc0, acc1, s2, r2, img, qacc,
    gxs, gxr, gmr, gyr, gzr, gall,
    qds, qdr, qxr, qf,
    wys, wyr, wzr, wall, back, shrink,
    dsem, rsem, fsem,
    s0s, s0r, s1s, s1r, s2s, s2r, izs, izr, iys, iyr, ifs,
    gxss, gxsr, gmss, gmsr, gyss, gysr, gzss, gzsr, gass, gasr,
    qdsem, qxss, qxsr, qfsem,
    wyss, wysr, wzss, wzsr, wxss, wxsr,
):
    nx, nc, nz, ny, iters = dims
    nxc, nblk = nx * nc, nx - 1
    near = [(dy, dx, dc) for dy in range(ny) for dx in range(nx) for dc in range(nc) if dy + dx + dc]
    near.sort(key=lambda o: -(min(o[0], ny - o[0]) + min(o[1], nx - o[1]) + 0.1 * o[2]))
    k = pt.shape[0]
    feats = pt.shape[1]
    half = feats // nc
    rank_half = f_in.shape[1]
    rows = dv.shape[0] // ny
    x, f, c = lax.axis_index("samples"), lax.axis_index("features"), lax.axis_index("rhs")
    z, y = lax.div(f, ny), lax.rem(f, ny)
    other = 1 - c
    j = c * nx + x

    def to_y(yy):
        return {"features": z * ny + yy}

    def to_z(zz):
        return {"features": zz * ny + y}

    def to_core():
        return {"rhs": other}

    def to_x(xx):
        return {"samples": xx}

    def to_j(jj):
        return {"samples": lax.rem(jj, nx), "rhs": lax.div(jj, nx)}

    def moved(offset):
        dy, dx, dc = offset
        return lax.rem(y + dy, ny), lax.rem(x + dx, nx), lax.rem(c + dc, nc)

    def to_near(yy, xx, cc):
        return {"samples": xx, "features": z * ny + yy, "rhs": cc}

    def copy(src, dst, ss, rs, dev):
        return pltpu.make_async_remote_copy(
            src_ref=src, dst_ref=dst, send_sem=ss, recv_sem=rs, device_id=dev, device_id_type=MESH
        )

    def start_all(ref, me, n, to, ss, rs):
        for d in range(1, n):
            other_one = lax.rem(me + d, n)
            copy(ref.at[me], ref.at[me], ss.at[d], rs.at[me], to(other_one)).start()

    def wait_all(ref, me, n, to, ss, rs):
        for d in range(1, n):
            other_one = lax.rem(me + d, n)
            copy(ref.at[other_one], ref.at[other_one], ss.at[d], rs.at[other_one], to(other_one)).wait_recv()

    def sent_all(ref, me, n, to, ss, rs):
        for d in range(1, n):
            other_one = lax.rem(me + d, n)
            copy(ref.at[me], ref.at[me], ss.at[d], rs.at[me], to(other_one)).wait_send()

    def total(ref, n):
        t = ref[0].astype(F32)
        for i in range(1, n):
            t = t + ref[i].astype(F32)
        return t

    def f_lanes(cc):
        return pl.ds(pl.multiple_of(cc * rank_half, LANES), rank_half)

    own_half = pl.ds(pl.multiple_of(c * half, LANES), half)

    loads = [
        pltpu.make_async_copy(d_hbm.at[pl.ds(i * rows, rows)], dv.at[pl.ds(i * rows, rows)], dsem.at[i])
        for i in range(ny)
    ]
    load_r = pltpu.make_async_copy(rt_in, rfull.at[c], dsem.at[ny])
    load_f = pltpu.make_async_copy(f_in, fall.at[:, f_lanes(c)], dsem.at[ny + 1])
    load_r.start()
    load_f.start()
    for load in loads:
        load.start()

    barrier = pltpu.get_barrier_semaphore()
    for d in range(1, nz):
        pl.semaphore_signal(barrier, inc=1, device_id=to_z(lax.rem(z + d, nz)), device_id_type=MESH)
    for offset in near:
        pl.semaphore_signal(barrier, inc=1, device_id=to_near(*moved(offset)), device_id_type=MESH)
    pl.semaphore_wait(barrier, nz - 1 + len(near))

    load_r.wait()
    send_r = copy(rfull.at[c], rfull.at[c], rsem.at[0], rsem.at[1], to_core())
    send_r.start()
    load_f.wait()
    send_f = copy(fall.at[:, f_lanes(c)], fall.at[:, f_lanes(c)], fsem.at[0], fsem.at[1], to_core())
    send_f.start()

    quarter = k // ny

    over_y = [(d, 0) for d in range(1, ny)]
    over_yc = [(d, 0) for d in range(1, ny)] + [(d, 1) for d in range(ny)]

    def sum_copy(n, offset, received=False):
        yy, cc = lax.rem(y + offset[0], ny), lax.rem(c + offset[1], nc)
        slot = cc * ny + yy if received else c * ny + y
        return copy(wys.at[cc, yy], wyr.at[slot], wyss.at[n], wysr.at[slot], to_near(yy, x, cc))

    def plane_sum(value, offsets):
        if offsets is over_y:
            wys[c] = value.reshape(wys.shape[1:])
        else:
            for cc in range(nc):
                wys[cc] = value[:, cc * LANES : (cc + 1) * LANES].reshape(wys.shape[1:])
        for n, offset in enumerate(offsets):
            sum_copy(n, offset).start()
        wyr[c * ny + y] = wys[c, y]

    def plane_exchange(offsets):
        for n, offset in enumerate(offsets):
            sum_copy(n, offset, True).wait_recv()
        if offsets is over_y:
            t = wyr[c * ny]
            for i in range(1, ny):
                t = t + wyr[c * ny + i]
            wzr[z] = t
        else:
            wzr[z] = total(wyr, nc * ny)
        start_all(wzr, z, nz, to_z, wzss, wzsr)

    def near_copy(n, offset, source):
        yy, xx, cc = moved(offset)
        if source:
            return copy(wall.at[cc * nx + xx, yy], wall.at[cc * nx + xx, yy], wxss.at[n], wxsr.at[cc * nx + xx, yy], to_near(yy, xx, cc))
        return copy(wall.at[j, y], wall.at[j, y], wxss.at[n], wxsr.at[j, y], to_near(yy, xx, cc))

    def plane_finish(offsets):
        wait_all(wzr, z, nz, to_z, wzss, wzsr)
        whole = total(wzr, nz)
        upper, lower = halves(whole)
        wall[j, y] = jnp.where((x == nblk) & (c == 1), lower.astype(F32), upper.astype(F32)).astype(BF16)
        for n, offset in enumerate(near):
            near_copy(n, offset, False).start()
        for n, offset in enumerate(near):
            near_copy(n, offset, True).wait_recv()
        for n, offset in enumerate(offsets):
            sum_copy(n, offset).wait_send()
        sent_all(wzr, z, nz, to_z, wzss, wzsr)
        for n, offset in enumerate(near):
            near_copy(n, offset, False).wait_send()

    def block(jj):
        return wall[jj].reshape(k, LANES)

    def gathered(slots):
        return jnp.concatenate([block(jj) for jj in slots], 1)

    def spread(scaled):
        return rows_fine(scaled, nt, fall[...])

    least = jnp.min(jnp.min(values[...], axis=1, keepdims=True), axis=0, keepdims=True)
    table = (1.0 + least) / (1.0 + values[...]) - 1.0
    for r in range(values.shape[0]):
        shrink[:, r * LANES : (r + 1) * LANES] = table[r : r + 1, :]
    copy(rfull.at[c], rfull.at[other], rsem.at[0], rsem.at[1], to_core()).wait_recv()
    rt[...] = rfull[...].reshape(k, feats)
    xt[...] = jnp.zeros_like(xt)

    @pl.when(x < nblk)
    def _():
        lanes = pl.ds(pl.multiple_of(c * rank_half + x * LANES, LANES), LANES)
        plane_sum(rows_fine(rt[...], nn, fall[:, lanes]), over_y)

    @pl.when(x == nblk)
    def _():
        plane_sum(jnp.zeros((k, LANES), F32), over_y)

    plane_exchange(over_y)
    plane_finish(over_y)
    copy(fall.at[:, f_lanes(c)], fall.at[:, f_lanes(other)], fsem.at[0], fsem.at[1], to_core()).wait_recv()
    send_r.wait_send()
    send_f.wait_send()
    yt[...] = gathered([cc * nx + b for cc in range(nc) for b in range(nblk)]).astype(F32)
    pt[...] = rt[...] + spread(yt[...] * shrink[...])
    for load in loads:
        load.wait()

    y_order = [d for d in (2, 1, 3) if d < ny]
    beside = (1, nz - 1)
    distant = sorted(range(2, nz - 1), key=lambda d: -min(d, nz - d))
    arriving = distant[::-1]
    pieces = [*distant, 0]
    pairs = [(n, pieces[n : n + 2]) for n in range(0, len(pieces), 2)]

    def along_z(d):
        return lax.rem(z + d, nz)

    def along_y(d):
        return lax.rem(y + d, ny)

    def products(narrow, parts, offsets):
        start = [pl.multiple_of(along_y(d) * rows + along_z(o) * LANES, LANES) for d in parts for o in offsets]
        part = nt(narrow, jnp.concatenate([dv[pl.ds(at, LANES), :] for at in start], 0))
        cut = [part[:, n * LANES : (n + 1) * LANES] for n in range(len(start))]
        return [(d, cut[n * len(offsets) : (n + 1) * len(offsets)]) for n, d in enumerate(parts)]

    def s0_copy(b, d):
        return copy(s0.at[b, d], r0.at[b, d], s0s.at[b, d], s0r.at[b, d], to_z(along_z(beside[b])))

    def s1_copy(d, n, count, received=False):
        at = pl.ds(n, count)
        back_slot = d - 1 if received else ny - d - 1
        return copy(s1.at[d - 1, at], r1.at[back_slot, at], s1s.at[d - 1, n], s1r.at[back_slot, n], to_y(along_y(d)))

    def s2_copy(n, d):
        return copy(s2.at[n], r2.at[z], s2s.at[n], s2r.at[z], to_z(along_z(d)))

    def iy_copy(d, zz, slot):
        return copy(img.at[y, zz], img.at[y, zz], iys.at[d, slot], iyr.at[y, zz], to_y(along_y(d)))

    def if_copy(b, d):
        yy = along_y(d)
        return copy(img.at[yy, z], img.at[yy, z], ifs.at[b, d], iyr.at[yy, z], to_z(along_z(beside[b])))

    def iteration(step, carry):
        narrow = pt[...].astype(BF16)
        order = [*y_order, 0]
        parts = [order[n : n + 2] for n in range(0, ny, 2)]

        def beside_products(some):
            made = products(narrow, some, beside)
            for d, cut in made:
                for b in range(2):
                    s0[b, d] = cut[b].astype(BF16)
            for d, _ in made:
                for b in range(2):
                    s0_copy(b, d).start()

        def y_products(some, n, offsets):
            sent = [o for o in offsets if o]
            made = products(narrow, some, offsets)
            for d, cut in made:
                for m, part in enumerate(cut):
                    if not d:
                        acc1[n + m] = part
                    elif offsets[m]:
                        s1[d - 1, n + m] = part.astype(BF16)
                    else:
                        acc0[d] = part
            for d, _ in made:
                if d and sent:
                    s1_copy(d, n, len(sent)).start()

        for some in parts:
            y_products(some, *pairs[0])
        for some in parts:
            beside_products(some)
        for n, offsets in pairs[1:]:
            for some in parts:
                y_products(some, n, offsets)

        def y_summed(n, offsets):
            sent = [o for o in offsets if o]
            if sent:
                for d in range(1, ny):
                    s1_copy(d, n, len(sent), True).wait_recv()
            for m, o in enumerate(sent):
                tot = acc1[n + m]
                for d in range(1, ny):
                    tot = tot + r1[d - 1, n + m].astype(F32)
                s2[n + m] = tot.astype(BF16)
            for m, o in enumerate(sent):
                s2_copy(n + m, o).start()

        if len(pairs) > 1:
            y_summed(*pairs[0])
        last = len(distant)
        for d in [*y_order, 0]:
            for b in range(2):
                s0_copy(b, d).wait_recv()
            from_sides = r0[0, d].astype(F32) + r0[1, d].astype(F32)
            if d:
                s1[d - 1, last] = (acc0[d] + from_sides).astype(BF16)
                s1_copy(d, last, 1).start()
            else:
                acc1[last] += from_sides
        for n, offsets in pairs[1:] if len(pairs) > 1 else pairs:
            y_summed(n, offsets)
        mine = acc1[last]
        for d in range(1, ny):
            s1_copy(d, last, 1, True).wait_recv()
            mine = mine + r1[d - 1, last].astype(F32)
        for d in arriving[::-1]:
            zz = along_z(d)
            copy(s2.at[0], r2.at[zz], s2s.at[0], s2r.at[zz], to_z(zz)).wait_recv()
            mine = mine + r2[zz].astype(F32)

        img[y, z] = mine.astype(BF16)
        for d in y_order:
            iy_copy(d, z, 0).start()
        for d in [*distant, *beside]:
            copy(img.at[y, z], img.at[y, z], izs.at[d], izr.at[z], to_z(along_z(d))).start()

        lanes = pl.ds(pl.multiple_of(j * LANES, LANES), LANES)
        p_own, r_own = pt[:, lanes], rt[:, lanes]
        both = jnp.concatenate([mine, p_own], 1)
        gc = jnp.concatenate([nt_fine(both, both), nt_fine(r_own, p_own)], 1)
        gxs[...] = gc.reshape(gxs.shape)

        def gx_copy(d):
            jj = lax.rem(j + d, nxc)
            return copy(gxs.at[jj], gxr.at[j], gxss.at[d], gxsr.at[j], to_j(jj))

        def gm_copy(n, offset, received=False):
            yy, xx, cc = moved(offset)
            jj = cc * nx + xx
            slot = jj * ny + yy if received else j * ny + y
            return copy(gxs.at[jj], gmr.at[slot], gmss.at[n], gmsr.at[slot], to_near(yy, xx, cc))

        @pl.when(step + 1 < iters)
        def _():
            for d in range(1, nxc):
                gx_copy(d).start()
            gxr[j] = gxs[j]

        @pl.when(step + 1 == iters)
        def _():
            for n, offset in enumerate(near):
                gm_copy(n, offset).start()
            gmr[j * ny + y] = gxs[j]

        def arrived(d):
            zz = along_z(d)
            copy(img.at[y, zz], img.at[y, zz], izs.at[d], izr.at[zz], to_z(zz)).wait_recv()

        def forward(d):
            arrived(d)
            for e in y_order:
                iy_copy(e, along_z(d), d).start()

        def y_arrived(d, zz):
            yy = along_y(d)
            copy(img.at[yy, zz], img.at[yy, zz], iys.at[d, 0], iyr.at[yy, zz], to_y(yy)).wait_recv()

        def project(yy):
            flat = jnp.concatenate([img[yy, zz] for zz in range(nz)], 1)
            return nn(flat, dv[pl.ds(pl.multiple_of(yy * rows, rows), rows), :])

        for d in y_order[::-1]:
            y_arrived(d, z)
            for b in range(2):
                if_copy(b, d).start()
        for d in arriving[:2]:
            forward(d)
        for d in arriving[2:]:
            forward(d)
        @pl.when(step + 1 < iters)
        def _():
            wait_all(gxr, j, nxc, to_j, gxss, gxsr)
            gyr[y] = total(gxr, nxc)
            start_all(gyr, y, ny, to_y, gyss, gysr)

        @pl.when(step + 1 == iters)
        def _():
            for n, offset in enumerate(near):
                gm_copy(n, offset, True).wait_recv()
            gzr[z] = total(gmr, nxc * ny)
            start_all(gzr, z, nz, to_z, gzss, gzsr)

        for d in beside:
            arrived(d)
        qacc[...] = project(y)
        for d in [e for e in (1, 3, 2) if e < ny]:
            if d == y_order[0]:
                @pl.when(step + 1 < iters)
                def _():
                    wait_all(gyr, y, ny, to_y, gyss, gysr)
                    gzr[z] = total(gyr, ny)
                    start_all(gzr, z, nz, to_z, gzss, gzsr)

            for o in range(1, nz):
                y_arrived(d, along_z(o))
            qacc[...] += project(along_y(d))

        for h in range(nc):
            qds[h] = qacc[:, h * half : (h + 1) * half]
        qd = copy(qds.at[other], qdr, qdsem.at[0], qdsem.at[1], to_core())
        qd.start()
        def sums_along_x():
            qd.wait_recv()
            qxr[x] = (qds[c] + qdr[...]).astype(BF16)
            start_all(qxr, x, nx, to_x, qxss, qxsr)

        def gram_to_all():
            wait_all(gzr, z, nz, to_z, gzss, gzsr)
            gall[j] = total(gzr, nz)
            start_all(gall, j, nxc, to_j, gass, gasr)

        @pl.when(step + 1 < iters)
        def _():
            sums_along_x()
            gram_to_all()

        @pl.when(step + 1 == iters)
        def _():
            gram_to_all()
            sums_along_x()

        def step_coefficient():
            wait_all(gall, j, nxc, to_j, gass, gasr)
            gc = gall[...].reshape(k, 2 * k)
            inv = inverse(gc[:, :k])
            back[...] = nn_fine(gc[:, k:], inv)
            return inv

        def advance():
            old = tall(pt[...])
            xt[...] += nn(wide(back[...]), old)
            return old

        def join_halves():
            copy(qf.at[other], qf.at[other], qfsem.at[0], qfsem.at[1], to_core()).wait_recv()
            qt[...] = jnp.concatenate([qf[h] for h in range(nc)], 1) + pt[...]

        @pl.when(step + 1 == iters)
        def _():
            step_coefficient()

        wait_all(qxr, x, nx, to_x, qxss, qxsr)
        qf[c] = total(qxr, nx)
        qfc = copy(qf.at[c], qf.at[c], qfsem.at[0], qfsem.at[1], to_core())
        qfc.start()

        @pl.when(step + 1 == iters)
        def _():
            advance()
            join_halves()
            rt[...] -= nn_fine(back[...], qt[...])

        @pl.when(step + 1 < iters)
        def _():
            q_half = qf[c] + pt[:, own_half]

            @pl.when(x < nblk)
            def _():
                lanes = pl.ds(pl.multiple_of(x * (nc * LANES), nc * LANES), nc * LANES)
                plane_sum(rows_fine(q_half, nn, fall[own_half, lanes]), over_yc)

            @pl.when(x == nblk)
            def _():
                both = jnp.concatenate([nt_fine(rt[:, own_half], q_half), nt_fine(q_half, q_half)], 1)
                plane_sum(jnp.concatenate([both] * nc, 1), over_yc)

            join_halves()
            plane_exchange(over_yc)
            inv = step_coefficient()
            gp[...] = tall(nn(wide(inv), advance()))
            rt[...] -= nn_fine(back[...], qt[...])
            plane_finish(over_yc)
            image = gathered([cc * nx + b for b in range(nblk) for cc in range(nc)])
            small = block(nx - 1).astype(F32) + block(nx * nc - 1).astype(F32)
            weighted = image.astype(F32) * shrink[...]
            inner = nt(jnp.concatenate([*halves(yt[...] * shrink[...]), *halves(weighted)], 0), image)
            proj = yt[...] - rows_fine(back[...], nn, image)
            yt[...] = proj
            grown = small[:, k:] + inner[2 * k : 3 * k] + inner[3 * k :]
            cross = small[:, :k] + inner[:k] + inner[k : 2 * k] - nn_fine(back[...], grown)
            pt[...] = rt[...] + spread(proj * shrink[...]) - nn(wide(cross), gp[...])

        for d in range(ny):
            for b in range(2):
                s0_copy(b, d).wait_send()
        for n, offsets in pairs:
            sent = [o for o in offsets if o]
            for d in range(1, ny):
                if sent:
                    s1_copy(d, n, len(sent)).wait_send()
            for m, o in enumerate(sent):
                s2_copy(n + m, o).wait_send()
        for d in range(1, ny):
            s1_copy(d, last, 1).wait_send()
            for b in range(2):
                if_copy(b, d).wait_send()
            for slot in [0, *distant]:
                iy_copy(d, z, slot).wait_send()
        for d in range(1, nz):
            copy(img.at[y, z], img.at[y, z], izs.at[d], izr.at[z], to_z(along_z(d))).wait_send()
        @pl.when(step + 1 < iters)
        def _():
            for d in range(1, nxc):
                gx_copy(d).wait_send()
            sent_all(gyr, y, ny, to_y, gyss, gysr)

        @pl.when(step + 1 == iters)
        def _():
            for n, offset in enumerate(near):
                gm_copy(n, offset).wait_send()

        sent_all(gzr, z, nz, to_z, gzss, gzsr)
        sent_all(gall, j, nxc, to_j, gass, gasr)
        qd.wait_send()
        sent_all(qxr, x, nx, to_x, qxss, qxsr)
        qfc.wait_send()
        return carry

    lax.fori_loop(0, iters, iteration, 0)
    mine_rows = pl.ds(pl.multiple_of(c * (k // nc), k // nc), k // nc)
    out[0] = xt[mine_rows, :]
    out[1] = rt[mine_rows, :]


def shards(sizes, design, right_side, factor, nystrom_values):
    nx, nf, nc, ny = sizes
    nz = nf // ny
    nxc = nx * nc
    samples, feats = design.shape
    k = right_side.shape[1] * nc
    rank_half = factor.shape[1]
    vmem = pl.BlockSpec(memory_space=pltpu.VMEM)
    anywhere = pl.BlockSpec(memory_space=pl.ANY)
    dma = pltpu.SemaphoreType.DMA
    piece = (k // nxc, 2 * k)
    half = feats // nc
    scratch = [
        pltpu.VMEM((samples, feats), BF16),
        pltpu.VMEM((nc, k // nc, feats), F32),
        pltpu.VMEM((feats, nc * rank_half), BF16),
        pltpu.VMEM((k, feats), F32),
        pltpu.VMEM((k, feats), F32),
        pltpu.VMEM((k, feats), F32),
        pltpu.VMEM((k, nc * rank_half), F32),
        pltpu.VMEM((4 * k, feats), BF16),
        pltpu.VMEM((k, feats), F32),
        pltpu.VMEM((2, ny, k, LANES), BF16),
        pltpu.VMEM((2, ny, k, LANES), BF16),
        pltpu.VMEM((ny - 1, nz - 2, k, LANES), BF16),
        pltpu.VMEM((ny - 1, nz - 2, k, LANES), BF16),
        pltpu.VMEM((ny, k, LANES), F32),
        pltpu.VMEM((nz - 2, k, LANES), F32),
        pltpu.VMEM((nz - 3, k, LANES), BF16),
        pltpu.VMEM((nz, k, LANES), BF16),
        pltpu.VMEM((ny, nz, k, LANES), BF16),
        pltpu.VMEM((k, feats), F32),
        pltpu.VMEM((nxc, *piece), F32),
        pltpu.VMEM((nxc, *piece), F32),
        pltpu.VMEM((nxc * ny, *piece), F32),
        pltpu.VMEM((ny, *piece), F32),
        pltpu.VMEM((nz, *piece), F32),
        pltpu.VMEM((nxc, *piece), F32),
        pltpu.VMEM((nc, k, half), F32),
        pltpu.VMEM((k, half), F32),
        pltpu.VMEM((nx, k, half), BF16),
        pltpu.VMEM((nc, k, half), F32),
        pltpu.VMEM((nc, ny, k // ny, LANES), F32),
        pltpu.VMEM((nc * ny, k // ny, LANES), F32),
        pltpu.VMEM((nz, k // ny, LANES), F32),
        pltpu.VMEM((nxc, ny, k // ny, LANES), BF16),
        pltpu.VMEM((k, k), F32),
        pltpu.VMEM((1, nc * rank_half), F32),
        dma((ny + 2,)), dma((2,)), dma((2,)),
        dma((2, ny)), dma((2, ny)), dma((ny - 1, nz)), dma((ny - 1, nz)), dma((nz,)), dma((nz,)),
        dma((nz,)), dma((nz,)), dma((ny, nz)), dma((ny, nz)), dma((2, ny)),
        dma((nxc,)), dma((nxc,)), dma((nxc * ny,)), dma((nxc * ny,)), dma((ny,)), dma((ny,)),
        dma((nz,)), dma((nz,)), dma((nxc,)), dma((nxc,)),
        dma((2,)), dma((nx,)), dma((nx,)), dma((2,)),
        dma((nc * ny,)), dma((nc * ny,)), dma((nz,)), dma((nz,)), dma((nxc * ny,)), dma((nxc, ny)),
    ]
    out = pl.pallas_call(
        functools.partial(kernel, (nx, nc, nz, ny, ITERS)),
        out_shape=jax.ShapeDtypeStruct((2, k // nc, feats), F32),
        in_specs=[anywhere, anywhere, anywhere, vmem],
        out_specs=vmem,
        scratch_shapes=scratch,
        compiler_params=pltpu.CompilerParams(
            collective_id=0, has_side_effects=True, vmem_limit_bytes=56 * 2**20
        ),
        name="solve",
    )(design, right_side.T, factor, nystrom_values.reshape(-1, LANES))
    return out[0].T, out[1].T


def solution(mesh):
    placed = (P(("samples", "rhs"), "features"), P("features", "rhs"), P("features", "rhs"), P())
    nx, nf, nc = (mesh.shape[a] for a in ("samples", "features", "rhs"))
    ny = max(2, nf // 8)
    return jax.shard_map(
        functools.partial(shards, (nx, nf, nc, ny)),
        mesh=mesh,
        in_specs=placed,
        out_specs=(P("features", "rhs"), P("features", "rhs")),
        check_vma=False,
    )
```

```python
import functools

import jax
import jax.numpy as jnp
from jax import lax
from jax.experimental import pallas as pl
from jax.experimental.pallas import tpu as pltpu
from jax.sharding import PartitionSpec as P

ITERS = 3
LANES = 128
MESH = pl.DeviceIdType.MESH
F32 = jnp.float32
BF16 = jnp.bfloat16


def nt(a, b):
    return lax.dot_general(a, b, (((1,), (1,)), ((), ())), preferred_element_type=F32)


def nn(a, b):
    return lax.dot_general(a, b, (((1,), (0,)), ((), ())), preferred_element_type=F32)


def halves(v):
    upper = v.astype(BF16)
    lower = (v - upper.astype(F32)).astype(BF16)
    return upper, lower


def wide(a):
    upper, lower = halves(a)
    return jnp.concatenate([upper, upper, lower, lower], 1)


def tall(b):
    return jnp.concatenate(halves(b) * 2, 0)


def nn_fine(a, b):
    return nn(wide(a), tall(b))


def nt_fine(a, b):
    m, n = a.shape[0], b.shape[0]
    t = nt(jnp.concatenate(halves(a), 0), jnp.concatenate(halves(b), 0))
    return t[:m, :n] + t[:m, n:] + t[m:, :n] + t[m:, n:]


def rows_fine(a, op, b):
    m = a.shape[0]
    t = op(jnp.concatenate(halves(a), 0), b)
    return t[:m] + t[m:]


def inverse(a, width=8):
    n = a.shape[0]
    lane = lax.broadcasted_iota(jnp.int32, (1, n), 1)
    sub = lax.broadcasted_iota(jnp.int32, (n, 1), 0)
    for i in range(0, n, width):
        cols = [jnp.broadcast_to(a[:, i + t : i + t + 1], (n, n)) for t in range(width)]
        pivots = [[cols[t][i + r : i + r + 1, :] for t in range(width)] for r in range(width)]
        inside = (lane >= i) & (lane < i + width)
        rows = [jnp.where(lane == i + r, 1.0, jnp.where(inside, 0.0, a[i + r : i + r + 1, :])) for r in range(width)]
        for r in range(width):
            over = 1.0 / pivots[r][r]
            rows[r] = rows[r] * over
            for t in range(r + 1, width):
                pivots[r][t] = pivots[r][t] * over
            for q in range(width):
                if q != r:
                    factor = pivots[q][r]
                    rows[q] = rows[q] - factor * rows[r]
                    for t in range(r + 1, width):
                        pivots[q][t] = pivots[q][t] - factor * pivots[r][t]
        a = jnp.where(inside, 0.0, a)
        for r in range(width):
            a = a - cols[r] * rows[r]
        for r in range(width):
            a = jnp.where(sub == i + r, rows[r], a)
    return a


def kernel(
    dims,
    d_hbm, rt_in, f_in, values,
    out,
    dv, rfull, fall, pt, rt, xt, yt, gp, qt,
    s0, r0, s1, r1, acc0, acc1, s2, r2, img, qacc,
    gxs, gxr, gmr, gyr, gzr, gall,
    qds, qdr, qxr, qf,
    wys, wyr, wzr, wall, back, shrink,
    dsem, rsem, fsem,
    s0s, s0r, s1s, s1r, s2s, s2r, izs, izr, iys, iyr, ifs,
    gxss, gxsr, gmss, gmsr, gyss, gysr, gzss, gzsr, gass, gasr,
    qdsem, qxss, qxsr, qfsem,
    wyss, wysr, wzss, wzsr, wxss, wxsr,
):
    nx, nc, nz, ny, iters = dims
    nxc, nblk = nx * nc, nx - 1
    near = [(dy, dx, dc) for dy in range(ny) for dx in range(nx) for dc in range(nc) if dy + dx + dc]
    near.sort(key=lambda o: -(min(o[0], ny - o[0]) + min(o[1], nx - o[1]) + 0.1 * o[2]))
    k = pt.shape[0]
    feats = pt.shape[1]
    half = feats // nc
    rank_half = f_in.shape[1]
    rows = dv.shape[0] // ny
    x, f, c = lax.axis_index("samples"), lax.axis_index("features"), lax.axis_index("rhs")
    z, y = lax.div(f, ny), lax.rem(f, ny)
    other = 1 - c
    j = c * nx + x

    def to_y(yy):
        return {"features": z * ny + yy}

    def to_z(zz):
        return {"features": zz * ny + y}

    def to_core():
        return {"rhs": other}

    def to_x(xx):
        return {"samples": xx}

    def to_j(jj):
        return {"samples": lax.rem(jj, nx), "rhs": lax.div(jj, nx)}

    def moved(offset):
        dy, dx, dc = offset
        return lax.rem(y + dy, ny), lax.rem(x + dx, nx), lax.rem(c + dc, nc)

    def to_near(yy, xx, cc):
        return {"samples": xx, "features": z * ny + yy, "rhs": cc}

    def copy(src, dst, ss, rs, dev):
        return pltpu.make_async_remote_copy(
            src_ref=src, dst_ref=dst, send_sem=ss, recv_sem=rs, device_id=dev, device_id_type=MESH
        )

    def far_first(n, ring):
        return sorted(range(1, n), key=lambda d: -min(d % ring, ring - d % ring))

    def start_all(ref, me, n, to, ss, rs):
        for d in far_first(n, nx if to is to_j else n):
            other_one = lax.rem(me + d, n)
            copy(ref.at[me], ref.at[me], ss.at[d], rs.at[me], to(other_one)).start()

    def wait_all(ref, me, n, to, ss, rs):
        for d in range(1, n):
            other_one = lax.rem(me + d, n)
            copy(ref.at[other_one], ref.at[other_one], ss.at[d], rs.at[other_one], to(other_one)).wait_recv()

    def sent_all(ref, me, n, to, ss, rs):
        for d in range(1, n):
            other_one = lax.rem(me + d, n)
            copy(ref.at[me], ref.at[me], ss.at[d], rs.at[me], to(other_one)).wait_send()

    def total(ref, n):
        t = ref[0].astype(F32)
        for i in range(1, n):
            t = t + ref[i].astype(F32)
        return t

    def f_lanes(cc):
        return pl.ds(pl.multiple_of(cc * rank_half, LANES), rank_half)

    own_half = pl.ds(pl.multiple_of(c * half, LANES), half)

    loads = [
        pltpu.make_async_copy(d_hbm.at[pl.ds(i * rows, rows)], dv.at[pl.ds(i * rows, rows)], dsem.at[i])
        for i in range(ny)
    ]
    load_r = pltpu.make_async_copy(rt_in, rfull.at[c], dsem.at[ny])
    load_f = pltpu.make_async_copy(f_in, fall.at[:, f_lanes(c)], dsem.at[ny + 1])
    load_r.start()
    load_f.start()
    for load in loads:
        load.start()

    barrier = pltpu.get_barrier_semaphore()
    for d in range(1, nz):
        pl.semaphore_signal(barrier, inc=1, device_id=to_z(lax.rem(z + d, nz)), device_id_type=MESH)
    for offset in near:
        pl.semaphore_signal(barrier, inc=1, device_id=to_near(*moved(offset)), device_id_type=MESH)
    pl.semaphore_wait(barrier, nz - 1 + len(near))

    load_r.wait()
    send_r = copy(rfull.at[c], rfull.at[c], rsem.at[0], rsem.at[1], to_core())
    send_r.start()
    load_f.wait()
    send_f = copy(fall.at[:, f_lanes(c)], fall.at[:, f_lanes(c)], fsem.at[0], fsem.at[1], to_core())
    send_f.start()

    quarter = k // ny

    over_y = [(d, 0) for d in far_first(ny, ny)]
    over_yc = [(d, e) for d in [*far_first(ny, ny), 0] for e in range(nc) if d or e]

    def sum_copy(n, offset, received=False):
        yy, cc = lax.rem(y + offset[0], ny), lax.rem(c + offset[1], nc)
        slot = cc * ny + yy if received else c * ny + y
        return copy(wys.at[cc, yy], wyr.at[slot], wyss.at[n], wysr.at[slot], to_near(yy, x, cc))

    def plane_sum(value, offsets):
        if offsets is over_y:
            wys[c] = value.reshape(wys.shape[1:])
        else:
            for cc in range(nc):
                wys[cc] = value[:, cc * LANES : (cc + 1) * LANES].reshape(wys.shape[1:])
        for n, offset in enumerate(offsets):
            sum_copy(n, offset).start()
        wyr[c * ny + y] = wys[c, y]

    def plane_exchange(offsets):
        for n, offset in enumerate(offsets):
            sum_copy(n, offset, True).wait_recv()
        if offsets is over_y:
            t = wyr[c * ny]
            for i in range(1, ny):
                t = t + wyr[c * ny + i]
            wzr[z] = t
        else:
            wzr[z] = total(wyr, nc * ny)
        start_all(wzr, z, nz, to_z, wzss, wzsr)

    def near_copy(n, offset, source):
        yy, xx, cc = moved(offset)
        if source:
            return copy(wall.at[cc * nx + xx, yy], wall.at[cc * nx + xx, yy], wxss.at[n], wxsr.at[cc * nx + xx, yy], to_near(yy, xx, cc))
        return copy(wall.at[j, y], wall.at[j, y], wxss.at[n], wxsr.at[j, y], to_near(yy, xx, cc))

    def plane_finish(offsets):
        wait_all(wzr, z, nz, to_z, wzss, wzsr)
        whole = total(wzr, nz)
        upper, lower = halves(whole)
        wall[j, y] = jnp.where((x == nblk) & (c == 1), lower.astype(F32), upper.astype(F32)).astype(BF16)
        for n, offset in enumerate(near):
            near_copy(n, offset, False).start()
        for n, offset in enumerate(near):
            near_copy(n, offset, True).wait_recv()
        for n, offset in enumerate(offsets):
            sum_copy(n, offset).wait_send()
        sent_all(wzr, z, nz, to_z, wzss, wzsr)
        for n, offset in enumerate(near):
            near_copy(n, offset, False).wait_send()

    def block(jj):
        return wall[jj].reshape(k, LANES)

    def gathered(slots):
        return jnp.concatenate([block(jj) for jj in slots], 1)

    def spread(scaled):
        return rows_fine(scaled, nt, fall[...])

    least = jnp.min(jnp.min(values[...], axis=1, keepdims=True), axis=0, keepdims=True)
    table = (1.0 + least) / (1.0 + values[...]) - 1.0
    for r in range(values.shape[0]):
        shrink[:, r * LANES : (r + 1) * LANES] = table[r : r + 1, :]
    copy(rfull.at[c], rfull.at[other], rsem.at[0], rsem.at[1], to_core()).wait_recv()
    rt[...] = rfull[...].reshape(k, feats)
    xt[...] = jnp.zeros_like(xt)

    @pl.when(x < nblk)
    def _():
        lanes = pl.ds(pl.multiple_of(c * rank_half + x * LANES, LANES), LANES)
        plane_sum(rows_fine(rt[...], nn, fall[:, lanes]), over_y)

    @pl.when(x == nblk)
    def _():
        plane_sum(jnp.zeros((k, LANES), F32), over_y)

    plane_exchange(over_y)
    plane_finish(over_y)
    copy(fall.at[:, f_lanes(c)], fall.at[:, f_lanes(other)], fsem.at[0], fsem.at[1], to_core()).wait_recv()
    send_r.wait_send()
    send_f.wait_send()
    yt[...] = gathered([cc * nx + b for cc in range(nc) for b in range(nblk)]).astype(F32)
    pt[...] = rt[...] + spread(yt[...] * shrink[...])
    for load in loads:
        load.wait()

    y_order = [d for d in (2, 1, 3) if d < ny]
    beside = (1, nz - 1)
    distant = sorted(range(2, nz - 1), key=lambda d: -min(d, nz - d))
    arriving = distant[::-1]
    pieces = [*distant, 0]
    pairs = [(n, pieces[n : n + 2]) for n in range(0, len(pieces), 2)]

    def along_z(d):
        return lax.rem(z + d, nz)

    def along_y(d):
        return lax.rem(y + d, ny)

    def products(narrow, parts, offsets):
        start = [pl.multiple_of(along_y(d) * rows + along_z(o) * LANES, LANES) for d in parts for o in offsets]
        part = nt(narrow, jnp.concatenate([dv[pl.ds(at, LANES), :] for at in start], 0))
        cut = [part[:, n * LANES : (n + 1) * LANES] for n in range(len(start))]
        return [(d, cut[n * len(offsets) : (n + 1) * len(offsets)]) for n, d in enumerate(parts)]

    def s0_copy(b, d):
        return copy(s0.at[b, d], r0.at[b, d], s0s.at[b, d], s0r.at[b, d], to_z(along_z(beside[b])))

    def s1_copy(d, n, count, received=False):
        at = pl.ds(n, count)
        back_slot = d - 1 if received else ny - d - 1
        return copy(s1.at[d - 1, at], r1.at[back_slot, at], s1s.at[d - 1, n], s1r.at[back_slot, n], to_y(along_y(d)))

    def s2_copy(n, d):
        return copy(s2.at[n], r2.at[z], s2s.at[n], s2r.at[z], to_z(along_z(d)))

    def iy_copy(d, zz, slot):
        return copy(img.at[y, zz], img.at[y, zz], iys.at[d, slot], iyr.at[y, zz], to_y(along_y(d)))

    def if_copy(b, d):
        yy = along_y(d)
        return copy(img.at[yy, z], img.at[yy, z], ifs.at[b, d], iyr.at[yy, z], to_z(along_z(beside[b])))

    def iteration(step, carry):
        narrow = pt[...].astype(BF16)
        order = [*y_order, 0]
        parts = [order[n : n + 2] for n in range(0, ny, 2)]

        def beside_products(some):
            made = products(narrow, some, beside)
            for d, cut in made:
                for b in range(2):
                    s0[b, d] = cut[b].astype(BF16)
            for d, _ in made:
                for b in range(2):
                    s0_copy(b, d).start()

        def y_products(some, n, offsets):
            sent = [o for o in offsets if o]
            made = products(narrow, some, offsets)
            for d, cut in made:
                for m, part in enumerate(cut):
                    if not d:
                        acc1[n + m] = part
                    elif offsets[m]:
                        s1[d - 1, n + m] = part.astype(BF16)
                    else:
                        acc0[d] = part
            for d, _ in made:
                if d and sent:
                    s1_copy(d, n, len(sent)).start()

        for some in parts:
            y_products(some, *pairs[0])
        for some in parts:
            beside_products(some)
        for n, offsets in pairs[1:]:
            for some in parts:
                y_products(some, n, offsets)

        def y_summed(n, offsets):
            sent = [o for o in offsets if o]
            if sent:
                for d in range(1, ny):
                    s1_copy(d, n, len(sent), True).wait_recv()
            for m, o in enumerate(sent):
                tot = acc1[n + m]
                for d in range(1, ny):
                    tot = tot + r1[d - 1, n + m].astype(F32)
                s2[n + m] = tot.astype(BF16)
            for m, o in enumerate(sent):
                s2_copy(n + m, o).start()

        if len(pairs) > 1:
            y_summed(*pairs[0])
        last = len(distant)
        for d in [*y_order, 0]:
            for b in range(2):
                s0_copy(b, d).wait_recv()
            from_sides = r0[0, d].astype(F32) + r0[1, d].astype(F32)
            if d:
                s1[d - 1, last] = (acc0[d] + from_sides).astype(BF16)
                s1_copy(d, last, 1).start()
            else:
                acc1[last] += from_sides
        for n, offsets in pairs[1:] if len(pairs) > 1 else pairs:
            y_summed(n, offsets)
        mine = acc1[last]
        for d in range(1, ny):
            s1_copy(d, last, 1, True).wait_recv()
            mine = mine + r1[d - 1, last].astype(F32)
        for d in arriving[::-1]:
            zz = along_z(d)
            copy(s2.at[0], r2.at[zz], s2s.at[0], s2r.at[zz], to_z(zz)).wait_recv()
            mine = mine + r2[zz].astype(F32)

        img[y, z] = mine.astype(BF16)
        for d in y_order:
            iy_copy(d, z, 0).start()
        for d in [*distant, *beside]:
            copy(img.at[y, z], img.at[y, z], izs.at[d], izr.at[z], to_z(along_z(d))).start()

        lanes = pl.ds(pl.multiple_of(j * LANES, LANES), LANES)
        p_own, r_own = pt[:, lanes], rt[:, lanes]
        both = jnp.concatenate([mine, p_own], 1)
        gc = jnp.concatenate([nt_fine(both, both), nt_fine(r_own, p_own)], 1)
        gxs[...] = gc.reshape(gxs.shape)

        def gx_copy(d):
            jj = lax.rem(j + d, nxc)
            return copy(gxs.at[jj], gxr.at[j], gxss.at[d], gxsr.at[j], to_j(jj))

        def gm_copy(n, offset, received=False):
            yy, xx, cc = moved(offset)
            jj = cc * nx + xx
            slot = jj * ny + yy if received else j * ny + y
            return copy(gxs.at[jj], gmr.at[slot], gmss.at[n], gmsr.at[slot], to_near(yy, xx, cc))

        @pl.when(step + 1 < iters)
        def _():
            for d in far_first(nxc, nx):
                gx_copy(d).start()
            gxr[j] = gxs[j]

        @pl.when(step + 1 == iters)
        def _():
            for n, offset in enumerate(near):
                gm_copy(n, offset).start()
            gmr[j * ny + y] = gxs[j]

        def arrived(d):
            zz = along_z(d)
            copy(img.at[y, zz], img.at[y, zz], izs.at[d], izr.at[zz], to_z(zz)).wait_recv()

        def forward(d):
            arrived(d)
            for e in y_order:
                iy_copy(e, along_z(d), d).start()

        def y_arrived(d, zz):
            yy = along_y(d)
            copy(img.at[yy, zz], img.at[yy, zz], iys.at[d, 0], iyr.at[yy, zz], to_y(yy)).wait_recv()

        def project(yy):
            flat = jnp.concatenate([img[yy, zz] for zz in range(nz)], 1)
            return nn(flat, dv[pl.ds(pl.multiple_of(yy * rows, rows), rows), :])

        for d in y_order[::-1]:
            y_arrived(d, z)
            for b in range(2):
                if_copy(b, d).start()
        for d in arriving[:2]:
            forward(d)
        for d in arriving[2:]:
            forward(d)
        @pl.when(step + 1 < iters)
        def _():
            wait_all(gxr, j, nxc, to_j, gxss, gxsr)
            gyr[y] = total(gxr, nxc)
            start_all(gyr, y, ny, to_y, gyss, gysr)

        @pl.when(step + 1 == iters)
        def _():
            for n, offset in enumerate(near):
                gm_copy(n, offset, True).wait_recv()
            gzr[z] = total(gmr, nxc * ny)
            start_all(gzr, z, nz, to_z, gzss, gzsr)

        for d in beside:
            arrived(d)
        qacc[...] = project(y)
        for d in [e for e in (1, 3, 2) if e < ny]:
            if d == y_order[0]:
                @pl.when(step + 1 < iters)
                def _():
                    wait_all(gyr, y, ny, to_y, gyss, gysr)
                    gzr[z] = total(gyr, ny)
                    start_all(gzr, z, nz, to_z, gzss, gzsr)

            for o in range(1, nz):
                y_arrived(d, along_z(o))
            qacc[...] += project(along_y(d))

        for h in range(nc):
            qds[h] = qacc[:, h * half : (h + 1) * half]
        qd = copy(qds.at[other], qdr, qdsem.at[0], qdsem.at[1], to_core())
        qd.start()
        def sums_along_x():
            qd.wait_recv()
            qxr[x] = (qds[c] + qdr[...]).astype(BF16)
            start_all(qxr, x, nx, to_x, qxss, qxsr)

        def gram_to_all():
            wait_all(gzr, z, nz, to_z, gzss, gzsr)
            gall[j] = total(gzr, nz)
            start_all(gall, j, nxc, to_j, gass, gasr)

        @pl.when(step + 1 < iters)
        def _():
            sums_along_x()
            gram_to_all()

        @pl.when(step + 1 == iters)
        def _():
            gram_to_all()
            sums_along_x()

        def step_coefficient():
            wait_all(gall, j, nxc, to_j, gass, gasr)
            gc = gall[...].reshape(k, 2 * k)
            inv = inverse(gc[:, :k])
            back[...] = nn_fine(gc[:, k:], inv)
            return inv

        def advance():
            old = tall(pt[...])
            xt[...] += nn(wide(back[...]), old)
            return old

        def join_halves():
            copy(qf.at[other], qf.at[other], qfsem.at[0], qfsem.at[1], to_core()).wait_recv()
            qt[...] = jnp.concatenate([qf[h] for h in range(nc)], 1) + pt[...]

        @pl.when(step + 1 == iters)
        def _():
            step_coefficient()

        wait_all(qxr, x, nx, to_x, qxss, qxsr)
        qf[c] = total(qxr, nx)
        qfc = copy(qf.at[c], qf.at[c], qfsem.at[0], qfsem.at[1], to_core())
        qfc.start()

        @pl.when(step + 1 == iters)
        def _():
            advance()
            join_halves()
            rt[...] -= nn_fine(back[...], qt[...])

        @pl.when(step + 1 < iters)
        def _():
            q_half = qf[c] + pt[:, own_half]

            @pl.when(x < nblk)
            def _():
                lanes = pl.ds(pl.multiple_of(x * (nc * LANES), nc * LANES), nc * LANES)
                plane_sum(rows_fine(q_half, nn, fall[own_half, lanes]), over_yc)

            @pl.when(x == nblk)
            def _():
                both = jnp.concatenate([nt_fine(rt[:, own_half], q_half), nt_fine(q_half, q_half)], 1)
                plane_sum(jnp.concatenate([both] * nc, 1), over_yc)

            join_halves()
            plane_exchange(over_yc)
            inv = step_coefficient()
            gp[...] = tall(nn(wide(inv), advance()))
            rt[...] -= nn_fine(back[...], qt[...])
            plane_finish(over_yc)
            image = gathered([cc * nx + b for b in range(nblk) for cc in range(nc)])
            small = block(nx - 1).astype(F32) + block(nx * nc - 1).astype(F32)
            weighted = image.astype(F32) * shrink[...]
            inner = nt(jnp.concatenate([*halves(yt[...] * shrink[...]), *halves(weighted)], 0), image)
            proj = yt[...] - rows_fine(back[...], nn, image)
            yt[...] = proj
            grown = small[:, k:] + inner[2 * k : 3 * k] + inner[3 * k :]
            cross = small[:, :k] + inner[:k] + inner[k : 2 * k] - nn_fine(back[...], grown)
            pt[...] = rt[...] + spread(proj * shrink[...]) - nn(wide(cross), gp[...])

        for d in range(ny):
            for b in range(2):
                s0_copy(b, d).wait_send()
        for n, offsets in pairs:
            sent = [o for o in offsets if o]
            for d in range(1, ny):
                if sent:
                    s1_copy(d, n, len(sent)).wait_send()
            for m, o in enumerate(sent):
                s2_copy(n + m, o).wait_send()
        for d in range(1, ny):
            s1_copy(d, last, 1).wait_send()
            for b in range(2):
                if_copy(b, d).wait_send()
            for slot in [0, *distant]:
                iy_copy(d, z, slot).wait_send()
        for d in range(1, nz):
            copy(img.at[y, z], img.at[y, z], izs.at[d], izr.at[z], to_z(along_z(d))).wait_send()
        @pl.when(step + 1 < iters)
        def _():
            for d in range(1, nxc):
                gx_copy(d).wait_send()
            sent_all(gyr, y, ny, to_y, gyss, gysr)

        @pl.when(step + 1 == iters)
        def _():
            for n, offset in enumerate(near):
                gm_copy(n, offset).wait_send()

        sent_all(gzr, z, nz, to_z, gzss, gzsr)
        sent_all(gall, j, nxc, to_j, gass, gasr)
        qd.wait_send()
        sent_all(qxr, x, nx, to_x, qxss, qxsr)
        qfc.wait_send()
        return carry

    lax.fori_loop(0, iters, iteration, 0)
    mine_rows = pl.ds(pl.multiple_of(c * (k // nc), k // nc), k // nc)
    out[0] = xt[mine_rows, :]
    out[1] = rt[mine_rows, :]


def shards(sizes, design, right_side, factor, nystrom_values):
    nx, nf, nc, ny = sizes
    nz = nf // ny
    nxc = nx * nc
    samples, feats = design.shape
    k = right_side.shape[1] * nc
    rank_half = factor.shape[1]
    vmem = pl.BlockSpec(memory_space=pltpu.VMEM)
    anywhere = pl.BlockSpec(memory_space=pl.ANY)
    dma = pltpu.SemaphoreType.DMA
    piece = (k // nxc, 2 * k)
    half = feats // nc
    scratch = [
        pltpu.VMEM((samples, feats), BF16),
        pltpu.VMEM((nc, k // nc, feats), F32),
        pltpu.VMEM((feats, nc * rank_half), BF16),
        pltpu.VMEM((k, feats), F32),
        pltpu.VMEM((k, feats), F32),
        pltpu.VMEM((k, feats), F32),
        pltpu.VMEM((k, nc * rank_half), F32),
        pltpu.VMEM((4 * k, feats), BF16),
        pltpu.VMEM((k, feats), F32),
        pltpu.VMEM((2, ny, k, LANES), BF16),
        pltpu.VMEM((2, ny, k, LANES), BF16),
        pltpu.VMEM((ny - 1, nz - 2, k, LANES), BF16),
        pltpu.VMEM((ny - 1, nz - 2, k, LANES), BF16),
        pltpu.VMEM((ny, k, LANES), F32),
        pltpu.VMEM((nz - 2, k, LANES), F32),
        pltpu.VMEM((nz - 3, k, LANES), BF16),
        pltpu.VMEM((nz, k, LANES), BF16),
        pltpu.VMEM((ny, nz, k, LANES), BF16),
        pltpu.VMEM((k, feats), F32),
        pltpu.VMEM((nxc, *piece), F32),
        pltpu.VMEM((nxc, *piece), F32),
        pltpu.VMEM((nxc * ny, *piece), F32),
        pltpu.VMEM((ny, *piece), F32),
        pltpu.VMEM((nz, *piece), F32),
        pltpu.VMEM((nxc, *piece), F32),
        pltpu.VMEM((nc, k, half), F32),
        pltpu.VMEM((k, half), F32),
        pltpu.VMEM((nx, k, half), BF16),
        pltpu.VMEM((nc, k, half), F32),
        pltpu.VMEM((nc, ny, k // ny, LANES), F32),
        pltpu.VMEM((nc * ny, k // ny, LANES), F32),
        pltpu.VMEM((nz, k // ny, LANES), F32),
        pltpu.VMEM((nxc, ny, k // ny, LANES), BF16),
        pltpu.VMEM((k, k), F32),
        pltpu.VMEM((1, nc * rank_half), F32),
        dma((ny + 2,)), dma((2,)), dma((2,)),
        dma((2, ny)), dma((2, ny)), dma((ny - 1, nz)), dma((ny - 1, nz)), dma((nz,)), dma((nz,)),
        dma((nz,)), dma((nz,)), dma((ny, nz)), dma((ny, nz)), dma((2, ny)),
        dma((nxc,)), dma((nxc,)), dma((nxc * ny,)), dma((nxc * ny,)), dma((ny,)), dma((ny,)),
        dma((nz,)), dma((nz,)), dma((nxc,)), dma((nxc,)),
        dma((2,)), dma((nx,)), dma((nx,)), dma((2,)),
        dma((nc * ny,)), dma((nc * ny,)), dma((nz,)), dma((nz,)), dma((nxc * ny,)), dma((nxc, ny)),
    ]
    out = pl.pallas_call(
        functools.partial(kernel, (nx, nc, nz, ny, ITERS)),
        out_shape=jax.ShapeDtypeStruct((2, k // nc, feats), F32),
        in_specs=[anywhere, anywhere, anywhere, vmem],
        out_specs=vmem,
        scratch_shapes=scratch,
        compiler_params=pltpu.CompilerParams(
            collective_id=0, has_side_effects=True, vmem_limit_bytes=56 * 2**20
        ),
        name="solve",
    )(design, right_side.T, factor, nystrom_values.reshape(-1, LANES))
    return out[0].T, out[1].T


def solution(mesh):
    placed = (P(("samples", "rhs"), "features"), P("features", "rhs"), P("features", "rhs"), P())
    nx, nf, nc = (mesh.shape[a] for a in ("samples", "features", "rhs"))
    ny = max(2, nf // 8)
    return jax.shard_map(
        functools.partial(shards, (nx, nf, nc, ny)),
        mesh=mesh,
        in_specs=placed,
        out_specs=(P("features", "rhs"), P("features", "rhs")),
        check_vma=False,
    )
```
